1024 devices in a mesh: gx: 16 (over y, z_hi), gy: 16 (over z_lo, core), gz: 4 (over x).
Axes of the slice: x: 4, y: 8, z: 16 (z_hi: 2, z_lo: 8; z = z_hi * 8 + z_lo), core: 2. Of those that a mesh axis runs over, the one named last changes fastest.
Arguments:
- gas_state: float32 [5, 128, 256, 512], P(None, 'gx', 'gy', 'gz'), may hold values from -6 to 6, as said below
- section_start: float32 [5, 128, 256, 512], P(None, 'gx', 'gy', 'gz'), may hold values from -6 to 6
- drop_cell: int32 [16, 16, 4, 16, 128], P('gx', 'gy', 'gz'), may hold values from 0 to 8191
- block_tile: int32 [16, 16, 4, 16], P('gx', 'gy', 'gz'), may hold values from 0 to 1, as said below
- droplets_per_block: int32 [16, 16, 4, 16], P('gx', 'gy', 'gz'), may hold values from 0 to 128, as said below
- drop_frac: float32 [16, 16, 4, 3, 16, 128], P('gx', 'gy', 'gz'), may hold values from -0.5 to 0.5
- drop_vel: float32 [16, 16, 4, 3, 16, 128], P('gx', 'gy', 'gz'), may hold values from -6 to 6
- drop_mass: float32 [16, 16, 4, 16, 128], P('gx', 'gy', 'gz'), may hold values from 0.1 to 4
- drop_temp: float32 [16, 16, 4, 16, 128], P('gx', 'gy', 'gz'), may hold values from -6 to 6
Outputs:
- new_state: float32 [5, 128, 256, 512], P(None, 'gx', 'gy', 'gz')
The draws below stay inside these ranges and needn't reach their ends.
Inputs may be any that keep to these rules, and one draw needn't show every extreme that they name: `gas_state`: component 0 (density) lies between 0.3 and 3.4. `drop_cell`: encodes the cell (x, y, z) within the block's tile as (x * 8 + y) * 128 + z. `block_tile`: nondecreasing along a device's blocks; blocks with count 0 carry tile 1 (the last tile). `droplets_per_block`: on each device the blocks with a positive count come first and every later block has count 0; each device has at least 4 live blocks, one of them with 128 droplets; some device has all 16 blocks live. Slot d of a block is live when d is below its count.
All inputs are finite; a program needn't handle non-finite values.
Results may differ from the reference program's by a relative error of at most 0.00057.
Values sent between devices are 32-bit elements; how exact they have to be, the bound alone decides.
No kernel may reach another device: no remote copies, remote signals or barrier semaphores. Data moves between devices by JAX's collectives and lax.ppermute only.
A program may use at most 32 MiB of HBM per device.

```python
import math
import jax
import jax.numpy as jnp
from jax import lax

CX = 8
CY = 16
CZ = 128
TS = 8
BLK = 128
NBLK = 16
NTILE = 2
NX = 128
NY = 256
NZ = 512
N_GX = 16
N_GY = 16
N_GZ = 4


def draw_gas_state(key, part):
    first_key, second_key = jax.random.split(jax.random.fold_in(key, 11))
    flow_shape = (4, NX, NY, NZ)
    velocity_temp = jnp.clip(jax.random.normal(second_key, flow_shape, jnp.float32), -6.0, 6.0)
    density = jnp.exp(0.3 * jnp.clip(jax.random.normal(first_key, (1, NX, NY, NZ), jnp.float32), -4.0, 4.0))
    return jnp.concatenate([density, velocity_temp], axis=0)


def block_layout(key):
    key_list = jax.random.split(jax.random.fold_in(key, 5), 6)
    devices = N_GX * N_GY * N_GZ
    span_size = NBLK - NBLK // 4
    first_draw = jax.random.randint(key_list[0], (devices,), 0, span_size + 1)
    second_draw = jax.random.randint(key_list[1], (devices,), 0, span_size + 1)
    live_blocks = NBLK // 4 + first_draw * second_draw // max(span_size, 1)
    chosen = jax.random.randint(key_list[2], (), 0, devices)
    live_blocks = jnp.where(jnp.arange(devices) == chosen, NBLK, live_blocks)
    positions = jnp.arange(NBLK, dtype=jnp.int32)[None, :]
    counts = jax.random.randint(key_list[3], (devices, NBLK), max(BLK // 2, 1), BLK + 1)
    full_block = jax.random.randint(key_list[4], (devices,), 0, live_blocks)
    counts = jnp.where(positions == full_block[:, None], BLK, counts)
    counts = jnp.where(positions < live_blocks[:, None], counts, 0)
    tile_ids = jax.random.randint(key_list[5], (devices, NBLK), 0, NTILE)
    tile_ids = jnp.where(positions < live_blocks[:, None], tile_ids, NTILE - 1)
    tile_ids = jnp.sort(tile_ids, axis=1)
    return (counts.reshape(N_GX, N_GY, N_GZ, NBLK).astype(jnp.int32), tile_ids.reshape(N_GX, N_GY, N_GZ, NBLK).astype(jnp.int32))


def draw_droplets_per_block(key, part):
    return block_layout(key)[0]


def draw_block_tile(key, part):
    return block_layout(key)[1]


def with_ends(entries, rng, smallest, largest):
    longest = entries.shape.index(max(entries.shape))
    spots = []
    for shift in (0, 1):
        where = [jax.random.randint(jax.random.fold_in(rng, axis), (), 0, length) for axis, length in enumerate(entries.shape)]
        where[longest] = (where[longest] + shift) % entries.shape[longest]
        spots.append(tuple(where))
    return entries.at[spots[0]].set(smallest).at[spots[1]].set(largest)


def block_levels(key, extent, pieces, smallest, top_value):
    loudness = 1.0
    for axis_at, shards_of in pieces:
        draws = jax.random.uniform(jax.random.fold_in(jax.random.fold_in(key, 6), axis_at), (shards_of,), jnp.float32, smallest / len(pieces), top_value / len(pieces))
        loudness = loudness * jnp.repeat(jnp.exp(draws), extent[axis_at] // shards_of).reshape((-1,) + (1,) * (len(extent) - 1 - axis_at))
    return loudness


def bell_draw(stream_key, shape, deviation, reach, cuts=(), held_as=jnp.bfloat16):
    loudness = block_levels(stream_key, shape, cuts, -0.22, 0.18) if cuts else 1.0
    values = jax.random.normal(stream_key, shape, jnp.float32) * deviation * loudness
    return jnp.minimum(jnp.maximum(values, -reach), reach).astype(held_as)


def setup_inputs(seed: int = 0) -> dict:
    keys = jax.random.split(jax.random.key(seed), 10)
    return {
        "gas_state": draw_gas_state(jax.random.fold_in(keys[9], 71), 0),
        "section_start": bell_draw(keys[1], (5, NX, NY, NZ), 1.0, 6.0, ((1, 16), (2, 16), (3, 4)), jnp.float32),
        "drop_cell": with_ends(jax.random.randint(keys[2], (N_GX, N_GY, N_GZ, NBLK, BLK), 0, TS * TS * CZ), jax.random.fold_in(keys[2], 1), 0, (TS * TS * CZ) - 1).astype(jnp.int32),
        "block_tile": draw_block_tile(jax.random.fold_in(keys[9], 71), 0),
        "droplets_per_block": draw_droplets_per_block(jax.random.fold_in(keys[9], 71), 0),
        "drop_frac": jnp.clip(jax.random.uniform(keys[5], (N_GX, N_GY, N_GZ, 3, NBLK, BLK), jnp.float32, -0.5, 0.5) * block_levels(keys[5], (N_GX, N_GY, N_GZ, 3, NBLK, BLK), ((0, 16), (1, 16), (2, 4)), -0.4, 0.0), -0.5, 0.5),
        "drop_vel": bell_draw(keys[6], (N_GX, N_GY, N_GZ, 3, NBLK, BLK), 1.0, 6.0, ((0, 16), (1, 16), (2, 4)), jnp.float32),
        "drop_mass": jnp.clip(jnp.exp(math.log(4.0) - 3.6888794 * jax.random.uniform(keys[7], (N_GX, N_GY, N_GZ, NBLK, BLK), jnp.float32) ** block_levels(keys[7], (N_GX, N_GY, N_GZ, NBLK, BLK), ((0, 16), (1, 16), (2, 4)), -0.2, 0.2)), 0.1, 4.0),
        "drop_temp": bell_draw(keys[8], (N_GX, N_GY, N_GZ, NBLK, BLK), 1.0, 6.0, ((0, 16), (1, 16), (2, 4)), jnp.float32),
    }


PARCEL = 8.0
LATENT = 0.5
TIME_INCREMENT = 0.2
VISCOSITY = 0.5


def cut_windows(values, tile_size):
    number = (values.shape[0] - 2) // tile_size
    trailing = values.shape[1:]
    rest_pad = [(0, 0)] * len(trailing)
    leading = values[:number * tile_size].reshape((number, tile_size) + trailing)
    upper_rows = jnp.pad(values[tile_size:], [(0, tile_size - 2)] + rest_pad)
    upper_rows = upper_rows.reshape((number, tile_size) + trailing)[:, :2]
    return jnp.concatenate([leading, upper_rows], axis=1)


def join_windows(values, tile_size):
    number = values.shape[0]
    trailing = values.shape[2:]
    rest_pad = [(0, 0)] * len(trailing)
    leading = values[:, :tile_size].reshape((number * tile_size,) + trailing)
    leading = jnp.pad(leading, [(0, 2)] + rest_pad)
    upper_rows = jnp.pad(values[:, tile_size:], [(0, 0), (0, tile_size - 2)] + rest_pad)
    upper_rows = upper_rows.reshape((number * tile_size,) + trailing)
    upper_rows = jnp.pad(upper_rows, [(tile_size, 0)] + rest_pad)[:number * tile_size + 2]
    return leading + upper_rows


def tile_footprints(padded, tile_size):
    arranged = cut_windows(jnp.moveaxis(padded, 1, 0), tile_size)
    arranged = cut_windows(jnp.moveaxis(arranged, 3, 0), tile_size)
    arranged = jnp.transpose(arranged, (2, 0, 4, 3, 1, 5))
    return arranged.reshape(arranged.shape[0] * arranged.shape[1], -1, arranged.shape[5])


def tiles_to_padded(tile_sums, tiles_x, tile_rows_along_y, components, tile_size):
    foot_width = tile_size + 2
    arranged = tile_sums.reshape(tiles_x, tile_rows_along_y, components, foot_width, foot_width, tile_sums.shape[2])
    arranged = jnp.transpose(arranged, (0, 3, 1, 4, 2, 5))
    arranged = join_windows(arranged, tile_size)
    arranged = join_windows(jnp.moveaxis(arranged, 0, 2), tile_size)
    return jnp.transpose(arranged, (2, 1, 0, 3))


def spread(position, offset, length):
    places = jnp.arange(length, dtype=jnp.int32)[None, :, None]
    anchor = position[:, None, :]
    low_weight = (0.5 * (0.5 - offset) * (0.5 - offset))[:, None, :]
    middle = (0.75 - offset * offset)[:, None, :]
    higher = (0.5 * (0.5 + offset) * (0.5 + offset))[:, None, :]
    return (jnp.where(places == anchor, low_weight, 0.0) + jnp.where(places == anchor + 1, middle, 0.0)
            + jnp.where(places == anchor + 2, higher, 0.0))


def block_weights(drop_cells, offsets, tile_size, cells_z):
    plane_size = tile_size * cells_z
    pos_x = drop_cells // plane_size
    pos_y = (drop_cells // cells_z) % tile_size
    pos_z = drop_cells % cells_z
    foot_width = tile_size + 2
    weight_x = spread(pos_x, offsets[0], foot_width)
    weight_y = spread(pos_y, offsets[1], foot_width)
    planar = (weight_x[:, :, None, :] * weight_y[:, None, :, :]).reshape(
        drop_cells.shape[0], foot_width * foot_width, drop_cells.shape[1])
    upward_direction = spread(pos_z, offsets[2], cells_z + 2)
    return planar, upward_direction


def droplet_terms(gas_at, velocity, masses, temper, counts):
    slots = jnp.arange(masses.shape[1], dtype=jnp.int32)[None, :]
    alive_weight = jnp.where(slots < counts[:, None], PARCEL, 0.0)
    diameter = jnp.cbrt(masses)
    spalding = jax.nn.softplus(gas_at[:, 4] - temper)
    evaporation = diameter * jnp.log1p(spalding)
    drag_force = (diameter * gas_at[:, 0])[:, None, :] * (gas_at[:, 1:4] - velocity)
    heat_flux = diameter * (gas_at[:, 4] - temper)
    momentum = evaporation[:, None, :] * velocity - drag_force
    energy = -heat_flux - LATENT * evaporation
    stacked = jnp.concatenate([evaporation[:, None, :], momentum, energy[:, None, :]], axis=1)
    return stacked * alive_weight[:, None, :]


def device_sources(footprints, drop_cells, tile_ids, counts, offsets, velocity, masses, temper):
    blocks, block_size = drop_cells.shape
    planar, upward_direction = block_weights(drop_cells, offsets, TS, CZ)
    planar = lax.optimization_barrier(planar.astype(jnp.bfloat16)).astype(jnp.float32)
    upward_direction = lax.optimization_barrier(upward_direction.astype(jnp.bfloat16)).astype(jnp.float32)
    source_portions = jnp.take(footprints, tile_ids, axis=0).astype(jnp.float32)
    nearby_gas_values = jnp.einsum("gsy,gyn->gsn", source_portions, upward_direction)
    gas_at = jnp.sum(nearby_gas_values.reshape(blocks, 5, -1, block_size) * planar[:, None], axis=2)
    sources = droplet_terms(gas_at, jnp.transpose(velocity, (1, 0, 2)), masses, temper, counts)
    weight_scaled_terms = (planar[:, None] * sources[:, :, None, :]).astype(jnp.bfloat16)
    weight_scaled_terms = lax.optimization_barrier(weight_scaled_terms).astype(jnp.float32).reshape(blocks, -1, block_size)
    spread_sources = jnp.einsum("peh,pch->pec", weight_scaled_terms, upward_direction)
    owners = (tile_ids[:, None] == jnp.arange(footprints.shape[0], dtype=jnp.int32)[None, :]).astype(jnp.float32)
    return jnp.einsum("bt,bkz->tkz", owners, spread_sources, precision=lax.Precision.HIGHEST)


def neighbour(padded, dim_index, offset):
    slicer = [slice(None), slice(1, -1), slice(1, -1), slice(1, -1)]
    length = padded.shape[dim_index] - 2
    slicer[dim_index] = slice(1 + offset, 1 + offset + length)
    return padded[tuple(slicer)]


def advance(padded, gas_state, section_start, sources):
    laplace = -6.0 * gas_state
    advect = jnp.zeros_like(gas_state)
    for dim_index in (1, 2, 3):
        higher = neighbour(padded, dim_index, 1)
        lower_cells = neighbour(padded, dim_index, -1)
        laplace = laplace + higher + lower_cells
        advect = advect + gas_state[dim_index][None] * (higher - lower_cells) * 0.5
    return 0.75 * section_start + 0.25 * (gas_state + TIME_INCREMENT * (VISCOSITY * laplace - advect + sources))


def reference(gas_state, section_start, drop_cell, block_tile, droplets_per_block, drop_frac, drop_vel, drop_mass, drop_temp):
    padded = jnp.pad(gas_state, ((0, 0), (1, 1), (1, 1), (1, 1)), mode="wrap")
    rounded = lax.optimization_barrier(padded.astype(jnp.bfloat16))
    devices = N_GX * N_GY * N_GZ

    def flatten(values):
        return values.reshape((devices,) + values.shape[3:])

    inputs = (flatten(drop_cell), flatten(block_tile), flatten(droplets_per_block), flatten(drop_frac),
              flatten(drop_vel), flatten(drop_mass), flatten(drop_temp), jnp.arange(devices, dtype=jnp.int32))
    running = jnp.zeros((5, NX + 2, NY + 2, NZ + 2), jnp.float32)

    def deposit_device(running, device_item):
        drop_cells, tile_ids, counts, offsets, velocity, masses, temper, device = device_item
        corner_x = ((device // (N_GY * N_GZ)) * CX).astype(jnp.int32)
        corner_y = (((device // N_GZ) % N_GY) * CY).astype(jnp.int32)
        corner_z = ((device % N_GZ) * CZ).astype(jnp.int32)
        root = (jnp.zeros((), jnp.int32), corner_x, corner_y, corner_z)
        local_cells = lax.dynamic_slice(rounded, root, (5, CX + 2, CY + 2, CZ + 2))
        footprints = tile_footprints(local_cells, TS)
        tile_sums = device_sources(footprints, drop_cells, tile_ids, counts, offsets, velocity, masses, temper)
        spread_sources = tiles_to_padded(tile_sums, CX // TS, CY // TS, 5, TS)
        current = lax.dynamic_slice(running, root, spread_sources.shape)
        return lax.dynamic_update_slice(running, current + spread_sources, root), None

    running, ignored = lax.scan(deposit_device, running, inputs)
    for dim_index in (1, 2, 3):
        moved_axis = jnp.moveaxis(running, dim_index, 0)
        core_cells = moved_axis[1:-1].at[0].add(moved_axis[-1]).at[-1].add(moved_axis[0])
        running = jnp.moveaxis(core_cells, 0, dim_index)
    return advance(padded, gas_state, section_start, running)
```

```python
import jax
import jax.numpy as jnp
from jax import lax
from jax.experimental import pallas as pl
from jax.experimental.pallas import tpu as pltpu
from jax.sharding import PartitionSpec as P

PARCEL = 8.0
LATENT = 0.5
TIME_INCREMENT = 0.2
VISCOSITY = 0.5

AXES = ("gx", "gy", "gz")
F32 = jnp.float32
BF16 = jnp.bfloat16
I32 = jnp.int32
FAR_AWAY = -100

OWN = 128
HALO = 64


def swaps(shape):
    nx, ny, nz = shape

    def pairs(target):
        out = []
        for i in range(nx):
            for j in range(ny):
                for k in range(nz):
                    a, b, c = target(i, j, k)
                    out.append(((i * ny + j) * nz + k, (a * ny + b) * nz + c))
        return out

    def d_side(i, j, k):
        if j == 0:
            return (i ^ 1, ny - 1, k)
        if j == ny - 1:
            return (i ^ 1, 0, k)
        return (i, ((j - 1) ^ 1) + 1, k)

    return {
        "A": pairs(lambda i, j, k: (i ^ 1, j, k)),
        "B": pairs(lambda i, j, k: ((i + 2) % nx if i % 2 == 0 else (i - 2) % nx, j, k)),
        "C": pairs(lambda i, j, k: (i, j ^ 1, k)),
        "D": pairs(d_side),
        "up": pairs(lambda i, j, k: (i, j, (k + 1) % nz)),
        "down": pairs(lambda i, j, k: (i, j, (k - 1) % nz)),
    }


def places():
    i, j = lax.axis_index("gx"), lax.axis_index("gy")
    odd_i, odd_j = lax.rem(i, 2), lax.rem(j, 2)
    wrap = jnp.logical_or(j == 0, j == lax.axis_size("gy") - 1)
    return odd_i, odd_j, wrap


def rows(start, size, unit):
    return pl.ds(pl.multiple_of(start, unit), size)


def choose(cond, yes, no):
    pl.when(cond)(yes)
    pl.when(jnp.logical_not(cond))(no)


def pack_y(gas, to_c, to_d):
    _, odd_j, _ = places()

    def put(ref, y):
        for c in range(5):
            ref[c * 8 : c * 8 + 8, :] = gas[pl.ds(c * OWN + y, 8, stride=16), :]

    def even():
        put(to_c, 15)
        put(to_d, 0)

    def odd():
        put(to_c, 0)
        put(to_d, 15)

    choose(odd_j == 0, even, odd)


def pack_a(gas, from_c, from_d, to_a):
    odd_i, _, _ = places()
    near = (1 - odd_i) * 112
    for c in range(5):
        at = c * 48
        to_a[at : at + 16, :] = gas[rows(c * OWN + near, 16, 16), :]
        to_a[at + 16 : at + 32, :] = gas[rows(c * OWN + 112 - near, 16, 16), :]
        to_a[at + 32 : at + 40, :] = from_c[c * 8 : c * 8 + 8, :]
        to_a[at + 40 : at + 48, :] = from_d[c * 8 : c * 8 + 8, :]


def pack_b(from_a, from_d, after, to_b):
    del after
    odd_i, _, wrap = places()
    far = (1 - odd_i) * 7
    for c in range(5):
        to_b[c * 24 : c * 24 + 16, :] = from_a[c * 48 + 16 : c * 48 + 32, :]
        to_b[c * 24 + 16 : c * 24 + 24, :] = jnp.zeros((8, 128), F32)
        to_b[c * 24 + 16 : c * 24 + 17, :] = from_a[pl.ds(c * 48 + 32 + far, 1), :]

    def wrapped():
        for c in range(5):
            to_b[c * 24 + 17 : c * 24 + 18, :] = from_d[pl.ds(c * 8 + far, 1), :]

    def inner():
        for c in range(5):
            to_b[c * 24 + 17 : c * 24 + 18, :] = from_a[pl.ds(c * 48 + 40 + far, 1), :]

    choose(wrap, wrapped, inner)


def join_halo(gas, from_c, from_d, from_a, from_b, halo, z_low, z_high):
    odd_i, _, wrap = places()
    near = odd_i * 7
    for c in range(5):
        at = c * HALO
        halo[at : at + 16, :] = from_a[c * 48 : c * 48 + 16, :]
        halo[at + 16 : at + 32, :] = from_b[c * 24 : c * 24 + 16, :]
        halo[at + 32 : at + 40, :] = from_c[c * 8 : c * 8 + 8, :]
        halo[at + 40 : at + 48, :] = jnp.zeros((8, 128), F32)
        halo[at + 40 : at + 41, :] = from_a[pl.ds(c * 48 + 32 + near, 1), :]
        halo[at + 41 : at + 42, :] = from_b[c * 24 + 16 : c * 24 + 17, :]
        halo[at + 56 : at + 64, :] = jnp.zeros((8, 128), F32)
        halo[at + 57 : at + 58, :] = from_b[c * 24 + 17 : c * 24 + 18, :]
    halo[5 * HALO : 384, :] = jnp.zeros((384 - 5 * HALO, 128), F32)

    def wrapped():
        for c in range(5):
            halo[c * HALO + 48 : c * HALO + 56, :] = from_a[c * 48 + 40 : c * 48 + 48, :]
            halo[c * HALO + 56 : c * HALO + 57, :] = from_d[pl.ds(c * 8 + near, 1), :]

    def inner():
        for c in range(5):
            halo[c * HALO + 48 : c * HALO + 56, :] = from_d[c * 8 : c * 8 + 8, :]
            halo[c * HALO + 56 : c * HALO + 57, :] = from_a[pl.ds(c * 48 + 40 + near, 1), :]

    choose(wrap, wrapped, inner)
    for n in range(8):
        part = gas[n * 128 : n * 128 + 128, :] if n < 5 else halo[(n - 5) * 128 : (n - 4) * 128, :]
        turned = part.T
        z_low[n : n + 1, :] = turned[0:1, :]
        z_high[n : n + 1, :] = turned[127:128, :]


def three(place, anchor, offset):
    low = 0.5 * (0.5 - offset) * (0.5 - offset)
    middle = 0.75 - offset * offset
    high = 0.5 * (0.5 + offset) * (0.5 + offset)
    step = place - anchor
    return jnp.where(step == -1, low, jnp.where(step == 0, middle, jnp.where(step == 1, high, 0.0)))


def weigh(gas, cell, shift, frac, after, planar, vertical, part):
    del after
    odd_i, odd_j, _ = places()
    blocks = cell.shape[0]
    near_x, far_x = 8 - 9 * odd_i, 9 * odd_i - 1
    c_y, d_y = 16 - 17 * odd_j, 17 * odd_j - 1
    r = lax.broadcasted_iota(I32, (192, 128), 0)
    q = r & 15
    group = (r >> 4) - 8
    on_y = jnp.where(q < 8, q, jnp.where(q == 8, near_x, jnp.where(q == 9, far_x, FAR_AWAY)))
    place_x = jnp.where(group < 0, r >> 4, jnp.where(group == 0, near_x, jnp.where(group == 1, far_x, on_y)))
    place_y = jnp.where(group == 2, c_y, jnp.where(group == 3, d_y, q))
    s = lax.broadcasted_iota(I32, (144, 128), 0)
    place_z = jnp.where(s < 128, s, jnp.where(s == 128, -1, jnp.where(s == 129, 128, FAR_AWAY)))
    cells = gas[...].astype(BF16)
    for b in range(blocks):
        lanes = slice(b * 128, b * 128 + 128)
        at = cell[b : b + 1, :]
        wx = three(place_x, at >> 10, frac[b : b + 1, :])
        wy = three(place_y, ((at >> 7) & 7) + shift[b : b + 1, :], frac[blocks + b : blocks + b + 1, :])
        wz = three(place_z, at & 127, frac[2 * blocks + b : 2 * blocks + b + 1, :]).astype(BF16)
        flat = (wx * wy).astype(BF16)
        planar[0:192, lanes] = flat
        planar[192:256, lanes] = jnp.zeros((64, 128), BF16)
        vertical[0:144, lanes] = wz
        vertical[144:256, lanes] = jnp.zeros((112, 128), BF16)
        seen = jnp.dot(cells, wz[0:128, :], preferred_element_type=F32)
        own = flat[0:128, :].astype(F32)
        for c in range(5):
            part[c * blocks + b : c * blocks + b + 1, :] = jnp.sum(
                seen[c * OWN : c * OWN + OWN, :] * own, axis=0, keepdims=True
            )


def deposit(
    halo, z_below, z_above, planar, vertical, part, diameter, alive, vel, temp, sums, ghost_low, ghost_high,
    gas_at, source, weighted, total,
):
    blocks = diameter.shape[0]

    def z_rows(ref):
        v = ref[...]
        turned = pltpu.roll(v, 64, 1)
        side = jnp.concatenate(
            [v[5:6], turned[5:6], v[6:7], turned[6:7], v[7:8], jnp.zeros((3, 128), F32)], axis=0
        )
        return jnp.concatenate([v, side], axis=1)

    ends = jnp.concatenate([z_rows(z_below), z_rows(z_above)], axis=0).astype(BF16)
    at_ends = jnp.dot(ends, planar[...], preferred_element_type=F32)
    around = halo[0 : 5 * HALO, :].astype(BF16)
    for b in range(blocks):
        lanes = slice(b * 128, b * 128 + 128)
        seen = jnp.dot(around, vertical[0:128, lanes], preferred_element_type=F32)
        side = planar[128:192, lanes].astype(F32)
        edge = vertical[128:144, lanes].astype(F32)
        ended = at_ends[0:8, lanes] * edge[0:1, :] + at_ends[8:16, lanes] * edge[1:2, :]
        for c in range(5):
            n = c * blocks + b
            gas_at[n : n + 1, :] = (
                part[n : n + 1, :]
                + ended[c : c + 1, :]
                + jnp.sum(seen[c * HALO : c * HALO + HALO, :] * side, axis=0, keepdims=True)
            )
    d = diameter[...]
    live = alive[...]
    warm = gas_at[4 * blocks : 5 * blocks, :] - temp[...]
    soft = jnp.maximum(warm, 0.0) + jnp.log1p(jnp.exp(-jnp.abs(warm)))
    rate = d * jnp.log1p(soft)
    pull = d * gas_at[0:blocks, :]
    source[0:blocks, :] = rate * live
    for m in range(3):
        v = vel[m * blocks : (m + 1) * blocks, :]
        u = gas_at[(m + 1) * blocks : (m + 2) * blocks, :]
        source[(m + 1) * blocks : (m + 2) * blocks, :] = (rate * v - pull * (u - v)) * live
    source[4 * blocks : 5 * blocks, :] = (-(d * warm) - LATENT * rate) * live
    for b in range(blocks):
        lanes = slice(b * 128, b * 128 + 128)
        flat = planar[0:192, lanes].astype(F32)
        for c in range(5):
            scaled = (flat * source[c * blocks + b : c * blocks + b + 1, :]).astype(BF16)
            weighted[c * OWN : c * OWN + OWN, lanes] = scaled[0:128, :]
            weighted[640 + c * HALO : 640 + c * HALO + HALO, lanes] = scaled[128:192, :]
        weighted[960:1024, lanes] = jnp.zeros((64, 128), BF16)
    total[...] = lax.dot_general(
        weighted[...], vertical[...], (((1,), (1,)), ((), ())), preferred_element_type=F32
    )
    sums[...] = total[0:960, 0:128]
    for n in range(8):
        turned = total[n * 128 : n * 128 + 128, 128:256].T
        ghost_low[n : n + 1, :] = turned[0:1, :]
        ghost_high[n : n + 1, :] = turned[1:2, :]


def upright(below, above):
    z = lax.broadcasted_iota(I32, (128, 128), 0)
    return jnp.where(z == 0, below, jnp.where(z == 127, above, 0.0)).T


def fold_z(sums, below, above, own, sides, to_c, to_d):
    for n in range(8):
        extra = upright(below[n : n + 1, :], above[n : n + 1, :])
        if n < 5:
            own[n * OWN : n * OWN + OWN, :] = sums[n * OWN : n * OWN + OWN, :] + extra
            continue
        for half in range(2):
            c = (n - 5) * 2 + half
            if c > 4:
                continue
            at = 640 + c * HALO
            here = sums[at : at + HALO, :] + extra[half * 64 : half * 64 + 64, :]
            sides[c * 32 : c * 32 + 32, :] = here[0:32, :]
            to_c[c * 16 : c * 16 + 16, :] = here[32:48, :]
            to_d[c * 16 : c * 16 + 16, :] = here[48:64, :]


def fold_y(sides, from_c, from_d, to_a):
    _, odd_j, wrap = places()
    keep = jnp.where(wrap, 0.0, 1.0).astype(F32)
    y = lax.broadcasted_iota(I32, (16, 128), 0)
    c_y = 15 - 15 * odd_j
    at_c, at_d = y == c_y, y == 15 - c_y
    for c in range(5):
        for side in range(2):
            row = c * 16 + 8 + side
            to_a[c * 40 + side * 16 : c * 40 + side * 16 + 16, :] = (
                sides[c * 32 + side * 16 : c * 32 + side * 16 + 16, :]
                + jnp.where(at_c, from_c[row : row + 1, :], 0.0)
                + jnp.where(at_d, from_d[row : row + 1, :] * keep, 0.0)
            )
        to_a[c * 40 + 32 : c * 40 + 40, :] = from_d[c * 16 : c * 16 + 8, :]


def relay_b(from_a, from_d, after, to_b):
    del after
    _, odd_j, wrap = places()
    gate = jnp.where(wrap, 1.0, 0.0).astype(F32)
    at_d = lax.broadcasted_iota(I32, (16, 128), 0) == 15 * odd_j
    for c in range(5):
        to_b[c * 16 : c * 16 + 16, :] = from_a[c * 40 + 16 : c * 40 + 32, :] + jnp.where(
            at_d, from_d[c * 16 + 9 : c * 16 + 10, :] * gate, 0.0
        )


def stencil(gas, start, halo, z_below, z_above, own, from_c, from_d, after, out, upper):
    del after
    odd_i, odd_j, wrap = places()
    keep = jnp.where(wrap, 0.0, 1.0).astype(F32)
    y = lax.broadcasted_iota(I32, (16, 128), 0)
    z = lax.broadcasted_iota(I32, (16, 128), 1)
    c_y = 15 - 15 * odd_j
    at_c, at_d = y == c_y, y == 15 - c_y
    near = (1 - odd_i) * 7
    high_x, low_x = 16 * odd_i, 16 - 16 * odd_i
    high_y, low_y = 32 + 16 * odd_j, 48 - 16 * odd_j
    for c in range(5):
        upper[...] = upright(z_below[c : c + 1, :], z_above[c : c + 1, :])
        for x in range(8):
            at = c * OWN + x * 16
            g = gas[at : at + 16, :]
            if x < 7:
                x_up = gas[at + 16 : at + 32, :]
            else:
                x_up = halo[rows(c * HALO + high_x, 16, 16), :]
            if x > 0:
                x_down = gas[at - 16 : at, :]
            else:
                x_down = halo[rows(c * HALO + low_x, 16, 16), :]
            y_up = jnp.where(y == 15, halo[pl.ds(c * HALO + high_y + x, 1), :], pltpu.roll(g, 15, 0))
            y_down = jnp.where(y == 0, halo[pl.ds(c * HALO + low_y + x, 1), :], pltpu.roll(g, 1, 0))
            ends = upper[x * 16 : x * 16 + 16, :]
            z_up = jnp.where(z == 127, ends, pltpu.roll(g, 127, 1))
            z_down = jnp.where(z == 0, ends, pltpu.roll(g, 1, 1))
            laplace = -6.0 * g + (x_up + x_down) + (y_up + y_down) + (z_up + z_down)
            advect = 0.5 * (
                gas[OWN + x * 16 : OWN + x * 16 + 16, :] * (x_up - x_down)
                + gas[2 * OWN + x * 16 : 2 * OWN + x * 16 + 16, :] * (y_up - y_down)
                + gas[3 * OWN + x * 16 : 3 * OWN + x * 16 + 16, :] * (z_up - z_down)
            )
            across = jnp.where(wrap & (near == x), 1.0, 0.0).astype(F32)
            added = (
                own[at : at + 16, :]
                + jnp.where(at_c, from_c[c * 16 + x : c * 16 + x + 1, :], 0.0)
                + jnp.where(
                    at_d,
                    from_d[c * 16 + x : c * 16 + x + 1, :] * keep + from_d[c * 16 + 8 : c * 16 + 9, :] * across,
                    0.0,
                )
            )
            out[at : at + 16, :] = 0.75 * start[at : at + 16, :] + 0.25 * (
                g + TIME_INCREMENT * (VISCOSITY * laplace - advect + added)
            )


def finish(base, from_a, from_b, out):
    odd_i, odd_j, wrap = places()
    near = (1 - odd_i) * 112
    scale = 0.25 * TIME_INCREMENT
    out[...] = base[...]
    for c in range(5):
        at = rows(c * OWN + near, 16, 16)
        out[at, :] = out[at, :] + scale * from_a[c * 40 : c * 40 + 16, :]
        at = rows(c * OWN + 112 - near, 16, 16)
        out[at, :] = out[at, :] + scale * from_b[c * 16 : c * 16 + 16, :]

    def across(y):
        def add():
            for c in range(5):
                at = pl.ds(c * OWN + y, 8, stride=16)
                out[at, :] = out[at, :] + scale * from_a[c * 40 + 32 : c * 40 + 40, :]

        return add

    pl.when(wrap & (odd_j == 0))(across(0))
    pl.when(wrap & (odd_j == 1))(across(15))


def call(body, name, out_shapes, *operands, loose=(), scratch=(), flops=10000):
    whole = pl.BlockSpec(memory_space=pltpu.VMEM)
    anywhere = pl.BlockSpec(memory_space=pl.ANY)
    single = not isinstance(out_shapes, list)
    outs = [out_shapes] if single else out_shapes
    result = pl.pallas_call(
        body,
        name=name,
        out_shape=[jax.ShapeDtypeStruct(s, t) for s, t in outs],
        in_specs=[anywhere if n in loose else whole for n in range(len(operands))],
        out_specs=[whole] * len(outs),
        scratch_shapes=list(scratch),
        compiler_params=pltpu.CompilerParams(vmem_limit_bytes=24 * 1024 * 1024),
        cost_estimate=pl.CostEstimate(flops=flops, bytes_accessed=100000, transcendentals=0),
    )(*operands)
    return result[0] if single else result


def local(gas_state, section_start, drop_cell, block_tile, droplets_per_block, drop_frac, drop_vel, drop_mass, drop_temp):
    shape = tuple(lax.axis_size(a) for a in AXES)
    routes = swaps(shape)

    def send(values, route):
        return lax.ppermute(values, AXES, routes[route])

    blocks = drop_cell.shape[3]
    gas = gas_state.reshape(640, 128)
    start = section_start.reshape(640, 128)
    cell = drop_cell.reshape(blocks, 128)
    frac = drop_frac.reshape(3 * blocks, 128)
    vel = drop_vel.reshape(3 * blocks, 128)
    temp = drop_temp.reshape(blocks, 128)
    diameter = jnp.cbrt(drop_mass.reshape(blocks, 128))
    slots = lax.broadcasted_iota(I32, (blocks, 128), 1)
    alive = jnp.where(slots < droplets_per_block.reshape(blocks, 1), PARCEL, 0.0).astype(F32)
    shift = jnp.broadcast_to(8 * block_tile.reshape(blocks, 1), (blocks, 128)).astype(I32)

    to_c, to_d = call(pack_y, "pack_y", [((40, 128), F32)] * 2, gas)
    gas_c, gas_d = send(to_c, "C"), send(to_d, "D")
    to_a = call(pack_a, "pack_a", ((240, 128), F32), gas, gas_c, gas_d)
    gas_a = send(to_a, "A")
    planar, vertical, part = call(
        weigh,
        "weigh",
        [((256, blocks * 128), BF16), ((256, blocks * 128), BF16), ((5 * blocks, 128), F32)],
        gas, cell, shift, frac, to_a,
        loose=(4,), flops=1 << 32,
    )
    gas_b = send(call(pack_b, "pack_b", ((120, 128), F32), gas_a, gas_d, part, loose=(2,)), "B")
    halo, low, high = call(
        join_halo, "join_halo", [((384, 128), F32), ((8, 128), F32), ((8, 128), F32)],
        gas, gas_c, gas_d, gas_a, gas_b,
    )
    above, below = send(low, "down"), send(high, "up")
    sums, low, high = call(
        deposit, "deposit", [((960, 128), F32), ((8, 128), F32), ((8, 128), F32)],
        halo, below, above, planar, vertical, part, diameter, alive, vel, temp,
        scratch=[
            pltpu.VMEM((5 * blocks, 128), F32),
            pltpu.VMEM((5 * blocks, 128), F32),
            pltpu.VMEM((1024, blocks * 128), BF16),
            pltpu.VMEM((1024, 256), F32),
        ],
    )
    dep_above, dep_below = send(low, "down"), send(high, "up")
    own, sides, to_c, to_d = call(
        fold_z, "fold_z", [((640, 128), F32), ((160, 128), F32), ((80, 128), F32), ((80, 128), F32)],
        sums, dep_below, dep_above,
    )
    dep_c, dep_d = send(to_c, "C"), send(to_d, "D")
    to_a = call(fold_y, "fold_y", ((200, 128), F32), sides, dep_c, dep_d)
    dep_a = send(to_a, "A")
    base = call(
        stencil, "stencil", ((640, 128), F32),
        gas, start, halo, below, above, own, dep_c, dep_d, to_a,
        loose=(8,), scratch=[pltpu.VMEM((128, 128), F32)], flops=1 << 32,
    )
    dep_b = send(call(relay_b, "relay_b", ((80, 128), F32), dep_a, dep_d, base, loose=(2,)), "B")
    out = call(finish, "finish", ((640, 128), F32), base, dep_a, dep_b)
    return out.reshape(gas_state.shape)


def solution(mesh):
    in_specs = (
        P(None, "gx", "gy", "gz"),
        P(None, "gx", "gy", "gz"),
        P("gx", "gy", "gz", None, None),
        P("gx", "gy", "gz", None),
        P("gx", "gy", "gz", None),
        P("gx", "gy", "gz", None, None, None),
        P("gx", "gy", "gz", None, None, None),
        P("gx", "gy", "gz", None, None),
        P("gx", "gy", "gz", None, None),
    )
    return jax.shard_map(local, mesh=mesh, in_specs=in_specs, out_specs=P(None, "gx", "gy", "gz"), check_vma=False)
```

```python
import jax
import jax.numpy as jnp
from jax import lax
from jax.experimental import pallas as pl
from jax.experimental.pallas import tpu as pltpu
from jax.sharding import PartitionSpec as P


PARCEL = 8.0
LATENT = 0.5
TIME_INCREMENT = 0.2
VISCOSITY = 0.5

AXES = ("gx", "gy", "gz")
F32 = jnp.float32
BF16 = jnp.bfloat16
I32 = jnp.int32
FAR_AWAY = -100

OWN = 128
HALO = 64


def swaps(shape):
    nx, ny, nz = shape

    def pairs(target):
        out = []
        for i in range(nx):
            for j in range(ny):
                for k in range(nz):
                    there = target(i, j, k)
                    if there is not None:
                        a, b, c = there
                        out.append(((i * ny + j) * nz + k, (a * ny + b) * nz + c))
        return out

    def d_side(i, j, k):
        if j == 0:
            return (i ^ 1, ny - 1, k)
        if j == ny - 1:
            return (i ^ 1, 0, k)
        return (i, ((j - 1) ^ 1) + 1, k)

    def turn(i, j, k):
        if j in (0, ny - 1):
            return ((i + 2) % nx if i % 2 == 0 else (i - 2) % nx, j, k)
        return None

    return {
        "near": pairs(lambda i, j, k: (i ^ 1, j, k)),
        "far": pairs(lambda i, j, k: ((i - 1) % nx if i % 2 == 0 else (i + 1) % nx, j, k)),
        "turn": pairs(turn),
        "C": pairs(lambda i, j, k: (i, j ^ 1, k)),
        "D": pairs(d_side),
    }


def places():
    i, j = lax.axis_index("gx"), lax.axis_index("gy")
    odd_i, odd_j = lax.rem(i, 2), lax.rem(j, 2)
    wrap = jnp.logical_or(j == 0, j == lax.axis_size("gy") - 1)
    return odd_i, odd_j, wrap


def rows(start, size, unit):
    return pl.ds(pl.multiple_of(start, unit), size)


def post_ends(ref, low, high):
    k, n = lax.axis_index("gz"), ref.shape[0] // 8
    ref[...] = jnp.zeros(ref.shape, F32)
    up, down = lax.rem(k + 1, n) * 8, lax.rem(k + n - 1, n) * 8
    for row in range(8):
        ref[pl.ds(up + row, 1), :] = high(row)
        ref[pl.ds(down + row, 1), :] = low(row)


def get_ends(ref):
    k, n = lax.axis_index("gz"), ref.shape[0] // 8
    below = ref[rows(lax.rem(k + n - 1, n) * 8, 8, 8), :]
    above = ref[rows(lax.rem(k + 1, n) * 8, 8, 8), :]
    return below, above


def choose(cond, yes, no):
    pl.when(cond)(yes)
    pl.when(jnp.logical_not(cond))(no)


def pack_y(gas, to_c, to_d):
    _, odd_j, _ = places()

    def put(ref, y):
        for c in range(5):
            ref[c * 8 : c * 8 + 8, :] = gas[pl.ds(c * OWN + y, 8, stride=16), :]

    def even():
        put(to_c, 15)
        put(to_d, 0)

    def odd():
        put(to_c, 0)
        put(to_d, 15)

    choose(odd_j == 0, even, odd)


def pack_x(gas, from_c, from_d, to_near, to_far, to_turn):
    odd_i, _, _ = places()
    near = (1 - odd_i) * 7
    to_near[120:128, :] = jnp.zeros((8, 128), F32)
    to_far[80:96, :] = jnp.zeros((16, 128), F32)
    to_turn[...] = jnp.zeros((8, 128), F32)
    for c in range(5):
        to_near[c * 24 : c * 24 + 16, :] = gas[rows(c * OWN + near * 16, 16, 16), :]
        to_near[c * 24 + 16 : c * 24 + 24, :] = from_d[c * 8 : c * 8 + 8, :]
        to_near[120 + c : 121 + c, :] = from_c[pl.ds(c * 8 + near, 1), :]
        to_far[c * 16 : c * 16 + 16, :] = gas[rows(c * OWN + 112 - near * 16, 16, 16), :]
        to_far[80 + c : 81 + c, :] = from_c[pl.ds(c * 8 + 7 - near, 1), :]
        to_far[88 + c : 89 + c, :] = from_d[pl.ds(c * 8 + 7 - near, 1), :]
        to_turn[c : c + 1, :] = from_d[pl.ds(c * 8 + near, 1), :]


def join_halo(gas, from_c, from_d, from_near, from_far, from_turn, after, halo, ends):
    del after
    odd_i, _, wrap = places()
    near = odd_i * 7
    for c in range(5):
        at = c * HALO
        halo[at : at + 16, :] = from_near[c * 24 : c * 24 + 16, :]
        halo[at + 16 : at + 32, :] = from_far[c * 16 : c * 16 + 16, :]
        halo[at + 32 : at + 40, :] = from_c[c * 8 : c * 8 + 8, :]
        halo[at + 40 : at + 48, :] = jnp.zeros((8, 128), F32)
        halo[at + 40 : at + 41, :] = from_near[120 + c : 121 + c, :]
        halo[at + 41 : at + 42, :] = from_far[80 + c : 81 + c, :]
        halo[at + 56 : at + 64, :] = jnp.zeros((8, 128), F32)
    halo[5 * HALO : 384, :] = jnp.zeros((384 - 5 * HALO, 128), F32)

    def wrapped():
        for c in range(5):
            at = c * HALO + 48
            halo[at : at + 8, :] = from_near[c * 24 + 16 : c * 24 + 24, :]
            halo[at + 8 : at + 9, :] = from_d[pl.ds(c * 8 + near, 1), :]
            halo[at + 9 : at + 10, :] = from_turn[c : c + 1, :]

    def inner():
        for c in range(5):
            at = c * HALO + 48
            halo[at : at + 8, :] = from_d[c * 8 : c * 8 + 8, :]
            halo[at + 8 : at + 9, :] = from_near[pl.ds(c * 24 + 16 + near, 1), :]
            halo[at + 9 : at + 10, :] = from_far[88 + c : 89 + c, :]

    choose(wrap, wrapped, inner)
    turned = []
    for n in range(8):
        part = gas[n * 128 : n * 128 + 128, :] if n < 5 else halo[(n - 5) * 128 : (n - 4) * 128, :]
        turned.append(part.T)
    post_ends(ends, lambda n: turned[n][0:1, :], lambda n: turned[n][127:128, :])


def three(place, anchor, offset):
    low = 0.5 * (0.5 - offset) * (0.5 - offset)
    middle = 0.75 - offset * offset
    high = 0.5 * (0.5 + offset) * (0.5 + offset)
    step = place - anchor
    return jnp.where(step == -1, low, jnp.where(step == 0, middle, jnp.where(step == 1, high, 0.0)))


def weigh(gas, cell, shift, frac, after, planar, vertical, part):
    del after
    odd_i, odd_j, _ = places()
    blocks = cell.shape[0]
    near_x, far_x = 8 - 9 * odd_i, 9 * odd_i - 1
    c_y, d_y = 16 - 17 * odd_j, 17 * odd_j - 1
    r = lax.broadcasted_iota(I32, (192, 128), 0)
    q = r & 15
    group = (r >> 4) - 8
    on_y = jnp.where(q < 8, q, jnp.where(q == 8, near_x, jnp.where(q == 9, far_x, FAR_AWAY)))
    place_x = jnp.where(group < 0, r >> 4, jnp.where(group == 0, near_x, jnp.where(group == 1, far_x, on_y)))
    place_y = jnp.where(group == 2, c_y, jnp.where(group == 3, d_y, q))
    s = lax.broadcasted_iota(I32, (144, 128), 0)
    place_z = jnp.where(s < 128, s, jnp.where(s == 128, -1, jnp.where(s == 129, 128, FAR_AWAY)))
    cells = gas[...].astype(BF16)
    for b in range(blocks):
        lanes = slice(b * 128, b * 128 + 128)
        at = cell[b : b + 1, :]
        wx = three(place_x, at >> 10, frac[b : b + 1, :])
        wy = three(place_y, ((at >> 7) & 7) + shift[b : b + 1, :], frac[blocks + b : blocks + b + 1, :])
        wz = three(place_z, at & 127, frac[2 * blocks + b : 2 * blocks + b + 1, :]).astype(BF16)
        flat = (wx * wy).astype(BF16)
        planar[0:192, lanes] = flat
        planar[192:256, lanes] = jnp.zeros((64, 128), BF16)
        vertical[0:144, lanes] = wz
        vertical[144:256, lanes] = jnp.zeros((112, 128), BF16)
        seen = jnp.dot(cells, wz[0:128, :], preferred_element_type=F32)
        own = flat[0:128, :].astype(F32)
        for c in range(5):
            part[c * blocks + b : c * blocks + b + 1, :] = jnp.sum(
                seen[c * OWN : c * OWN + OWN, :] * own, axis=0, keepdims=True
            )


def deposit(
    halo, z_ends, planar, vertical, part, diameter, alive, vel, temp, sums, ghosts,
    gas_at, source, weighted, total,
):
    blocks = diameter.shape[0]

    below, above = get_ends(z_ends)

    def z_rows(v):
        turned = pltpu.roll(v, 64, 1)
        side = jnp.concatenate(
            [v[5:6], turned[5:6], v[6:7], turned[6:7], v[7:8], jnp.zeros((3, 128), F32)], axis=0
        )
        return jnp.concatenate([v, side], axis=1)

    ends = jnp.concatenate([z_rows(below), z_rows(above)], axis=0).astype(BF16)
    at_ends = jnp.dot(ends, planar[...], preferred_element_type=F32)
    around = halo[0 : 5 * HALO, :].astype(BF16)
    for b in range(blocks):
        lanes = slice(b * 128, b * 128 + 128)
        seen = jnp.dot(around, vertical[0:128, lanes], preferred_element_type=F32)
        side = planar[128:192, lanes].astype(F32)
        edge = vertical[128:144, lanes].astype(F32)
        ended = at_ends[0:8, lanes] * edge[0:1, :] + at_ends[8:16, lanes] * edge[1:2, :]
        for c in range(5):
            n = c * blocks + b
            gas_at[n : n + 1, :] = (
                part[n : n + 1, :]
                + ended[c : c + 1, :]
                + jnp.sum(seen[c * HALO : c * HALO + HALO, :] * side, axis=0, keepdims=True)
            )
    d = diameter[...]
    live = alive[...]
    warm = gas_at[4 * blocks : 5 * blocks, :] - temp[...]
    soft = jnp.maximum(warm, 0.0) + jnp.log1p(jnp.exp(-jnp.abs(warm)))
    rate = d * jnp.log1p(soft)
    pull = d * gas_at[0:blocks, :]
    source[0:blocks, :] = rate * live
    for m in range(3):
        v = vel[m * blocks : (m + 1) * blocks, :]
        u = gas_at[(m + 1) * blocks : (m + 2) * blocks, :]
        source[(m + 1) * blocks : (m + 2) * blocks, :] = (rate * v - pull * (u - v)) * live
    source[4 * blocks : 5 * blocks, :] = (-(d * warm) - LATENT * rate) * live
    for b in range(blocks):
        lanes = slice(b * 128, b * 128 + 128)
        flat = planar[0:192, lanes].astype(F32)
        for c in range(5):
            scaled = (flat * source[c * blocks + b : c * blocks + b + 1, :]).astype(BF16)
            weighted[c * OWN : c * OWN + OWN, lanes] = scaled[0:128, :]
            weighted[640 + c * HALO : 640 + c * HALO + HALO, lanes] = scaled[128:192, :]
        weighted[960:1024, lanes] = jnp.zeros((64, 128), BF16)
    total[...] = lax.dot_general(
        weighted[...], vertical[...], (((1,), (1,)), ((), ())), preferred_element_type=F32
    )
    sums[...] = total[0:960, 0:128]
    turned = [total[n * 128 : n * 128 + 128, 128:256].T for n in range(8)]
    post_ends(ghosts, lambda n: turned[n][0:1, :], lambda n: turned[n][1:2, :])


def upright(below, above):
    z = lax.broadcasted_iota(I32, (128, 128), 0)
    return jnp.where(z == 0, below, jnp.where(z == 127, above, 0.0)).T


def fold_z(sums, z_ends, own, sides, to_c, to_d):
    below, above = get_ends(z_ends)
    for n in range(8):
        extra = upright(below[n : n + 1, :], above[n : n + 1, :])
        if n < 5:
            own[n * OWN : n * OWN + OWN, :] = sums[n * OWN : n * OWN + OWN, :] + extra
            continue
        for half in range(2):
            c = (n - 5) * 2 + half
            if c > 4:
                continue
            at = 640 + c * HALO
            here = sums[at : at + HALO, :] + extra[half * 64 : half * 64 + 64, :]
            sides[c * 32 : c * 32 + 32, :] = here[0:32, :]
            to_c[c * 16 : c * 16 + 16, :] = here[32:48, :]
            to_d[c * 16 : c * 16 + 16, :] = here[48:64, :]


def fold_y(sides, from_c, from_d, to_near, to_far, to_turn):
    _, odd_j, wrap = places()
    keep = jnp.where(wrap, 0.0, 1.0).astype(F32)
    y = lax.broadcasted_iota(I32, (16, 128), 0)
    c_y = 15 - 15 * odd_j
    at_c, at_d = y == c_y, y == 15 - c_y
    to_turn[...] = jnp.zeros((8, 128), F32)
    for c in range(5):
        for side in range(2):
            row = c * 16 + 8 + side
            folded = (
                sides[c * 32 + side * 16 : c * 32 + side * 16 + 16, :]
                + jnp.where(at_c, from_c[row : row + 1, :], 0.0)
                + jnp.where(at_d, from_d[row : row + 1, :] * keep, 0.0)
            )
            if side == 0:
                to_near[c * 24 : c * 24 + 16, :] = folded
            else:
                to_far[c * 16 : c * 16 + 16, :] = folded
        to_near[c * 24 + 16 : c * 24 + 24, :] = from_d[c * 16 : c * 16 + 8, :]
        to_turn[c : c + 1, :] = from_d[c * 16 + 9 : c * 16 + 10, :]


def stencil(gas, start, halo, z_ends, own, from_c, from_d, after, out, upper):
    del after
    below, above = get_ends(z_ends)
    odd_i, odd_j, wrap = places()
    keep = jnp.where(wrap, 0.0, 1.0).astype(F32)
    y = lax.broadcasted_iota(I32, (16, 128), 0)
    z = lax.broadcasted_iota(I32, (16, 128), 1)
    c_y = 15 - 15 * odd_j
    at_c, at_d = y == c_y, y == 15 - c_y
    near = (1 - odd_i) * 7
    high_x, low_x = 16 * odd_i, 16 - 16 * odd_i
    high_y, low_y = 32 + 16 * odd_j, 48 - 16 * odd_j
    for c in range(5):
        upper[...] = upright(below[c : c + 1, :], above[c : c + 1, :])
        for x in range(8):
            at = c * OWN + x * 16
            g = gas[at : at + 16, :]
            if x < 7:
                x_up = gas[at + 16 : at + 32, :]
            else:
                x_up = halo[rows(c * HALO + high_x, 16, 16), :]
            if x > 0:
                x_down = gas[at - 16 : at, :]
            else:
                x_down = halo[rows(c * HALO + low_x, 16, 16), :]
            y_up = jnp.where(y == 15, halo[pl.ds(c * HALO + high_y + x, 1), :], pltpu.roll(g, 15, 0))
            y_down = jnp.where(y == 0, halo[pl.ds(c * HALO + low_y + x, 1), :], pltpu.roll(g, 1, 0))
            ends = upper[x * 16 : x * 16 + 16, :]
            z_up = jnp.where(z == 127, ends, pltpu.roll(g, 127, 1))
            z_down = jnp.where(z == 0, ends, pltpu.roll(g, 1, 1))
            laplace = -6.0 * g + (x_up + x_down) + (y_up + y_down) + (z_up + z_down)
            advect = 0.5 * (
                gas[OWN + x * 16 : OWN + x * 16 + 16, :] * (x_up - x_down)
                + gas[2 * OWN + x * 16 : 2 * OWN + x * 16 + 16, :] * (y_up - y_down)
                + gas[3 * OWN + x * 16 : 3 * OWN + x * 16 + 16, :] * (z_up - z_down)
            )
            across = jnp.where(wrap & (near == x), 1.0, 0.0).astype(F32)
            added = (
                own[at : at + 16, :]
                + jnp.where(at_c, from_c[c * 16 + x : c * 16 + x + 1, :], 0.0)
                + jnp.where(
                    at_d,
                    from_d[c * 16 + x : c * 16 + x + 1, :] * keep + from_d[c * 16 + 8 : c * 16 + 9, :] * across,
                    0.0,
                )
            )
            out[at : at + 16, :] = 0.75 * start[at : at + 16, :] + 0.25 * (
                g + TIME_INCREMENT * (VISCOSITY * laplace - advect + added)
            )


def finish(base, from_near, from_far, from_turn, out):
    odd_i, odd_j, wrap = places()
    near = (1 - odd_i) * 112
    scale = 0.25 * TIME_INCREMENT
    gate = jnp.where(wrap, scale, 0.0).astype(F32)
    at_d = lax.broadcasted_iota(I32, (16, 128), 0) == 15 * odd_j
    out[...] = base[...]
    for c in range(5):
        at = rows(c * OWN + near, 16, 16)
        out[at, :] = out[at, :] + scale * from_near[c * 24 : c * 24 + 16, :]
        at = rows(c * OWN + 112 - near, 16, 16)
        turned = jnp.where(at_d, from_turn[c : c + 1, :] * gate, 0.0)
        out[at, :] = out[at, :] + scale * from_far[c * 16 : c * 16 + 16, :] + turned

    def across(y):
        def add():
            for c in range(5):
                at = pl.ds(c * OWN + y, 8, stride=16)
                out[at, :] = out[at, :] + scale * from_near[c * 24 + 16 : c * 24 + 24, :]

        return add

    pl.when(wrap & (odd_j == 0))(across(0))
    pl.when(wrap & (odd_j == 1))(across(15))


def call(body, out_shapes, *operands, loose=(), scratch=(), flops=10000):
    whole = pl.BlockSpec(memory_space=pltpu.VMEM)
    anywhere = pl.BlockSpec(memory_space=pl.ANY)
    single = not isinstance(out_shapes, list)
    outs = [out_shapes] if single else out_shapes
    result = pl.pallas_call(
        body,
        out_shape=[jax.ShapeDtypeStruct(s, t) for s, t in outs],
        in_specs=[anywhere if n in loose else whole for n in range(len(operands))],
        out_specs=[whole] * len(outs),
        scratch_shapes=list(scratch),
        compiler_params=pltpu.CompilerParams(vmem_limit_bytes=24 * 1024 * 1024),
        cost_estimate=pl.CostEstimate(flops=flops, bytes_accessed=100000, transcendentals=0),
    )(*operands)
    return result[0] if single else result


def local(gas_state, section_start, drop_cell, block_tile, droplets_per_block, drop_frac, drop_vel, drop_mass, drop_temp):
    shape = tuple(lax.axis_size(a) for a in AXES)
    routes = swaps(shape)

    def send(values, route):
        return lax.ppermute(values, AXES, routes[route])

    def swap_ends(values):
        chunks = values.reshape(shape[2], 8, 128)
        return lax.all_to_all(chunks, "gz", 0, 0).reshape(values.shape)

    blocks = drop_cell.shape[3]
    ends_shape = ((8 * shape[2], 128), F32)
    gas = gas_state.reshape(640, 128)
    start = section_start.reshape(640, 128)
    cell = drop_cell.reshape(blocks, 128)
    frac = drop_frac.reshape(3 * blocks, 128)
    vel = drop_vel.reshape(3 * blocks, 128)
    temp = drop_temp.reshape(blocks, 128)
    diameter = jnp.cbrt(drop_mass.reshape(blocks, 128))
    slots = lax.broadcasted_iota(I32, (blocks, 128), 1)
    alive = jnp.where(slots < droplets_per_block.reshape(blocks, 1), PARCEL, 0.0).astype(F32)
    shift = jnp.broadcast_to(8 * block_tile.reshape(blocks, 1), (blocks, 128)).astype(I32)

    to_c, to_d = call(pack_y, [((40, 128), F32)] * 2, gas)
    gas_d, gas_c = send(to_d, "D"), send(to_c, "C")
    to_near, to_far, to_turn = call(
        pack_x, [((128, 128), F32), ((96, 128), F32), ((8, 128), F32)], gas, gas_c, gas_d
    )
    gas_near, gas_far = send(to_near, "near"), send(to_far, "far")
    gas_turn = send(to_turn, "turn")
    planar, vertical, part = call(
        weigh,
        [((256, blocks * 128), BF16), ((256, blocks * 128), BF16), ((5 * blocks, 128), F32)],
        gas, cell, shift, frac, to_near,
        loose=(4,), flops=1 << 32,
    )
    halo, ends = call(
        join_halo, [((384, 128), F32), ends_shape],
        gas, gas_c, gas_d, gas_near, gas_far, gas_turn, part,
        loose=(6,),
    )
    ends = swap_ends(ends)
    sums, ghosts = call(
        deposit, [((960, 128), F32), ends_shape],
        halo, ends, planar, vertical, part, diameter, alive, vel, temp,
        scratch=[
            pltpu.VMEM((5 * blocks, 128), F32),
            pltpu.VMEM((5 * blocks, 128), F32),
            pltpu.VMEM((1024, blocks * 128), BF16),
            pltpu.VMEM((1024, 256), F32),
        ],
    )
    own, sides, to_c, to_d = call(
        fold_z, [((640, 128), F32), ((160, 128), F32), ((80, 128), F32), ((80, 128), F32)],
        sums, swap_ends(ghosts),
    )
    dep_d, dep_c = send(to_d, "D"), send(to_c, "C")
    to_near, to_far, to_turn = call(
        fold_y, [((120, 128), F32), ((80, 128), F32), ((8, 128), F32)], sides, dep_c, dep_d
    )
    dep_near, dep_far = send(to_near, "near"), send(to_far, "far")
    dep_turn = send(to_turn, "turn")
    base = call(
        stencil, ((640, 128), F32),
        gas, start, halo, ends, own, dep_c, dep_d, to_near,
        loose=(7,), scratch=[pltpu.VMEM((128, 128), F32)], flops=1 << 32,
    )
    out = call(finish, ((640, 128), F32), base, dep_near, dep_far, dep_turn)
    return out.reshape(gas_state.shape)


def solution(mesh):
    in_specs = (
        P(None, "gx", "gy", "gz"),
        P(None, "gx", "gy", "gz"),
        P("gx", "gy", "gz", None, None),
        P("gx", "gy", "gz", None),
        P("gx", "gy", "gz", None),
        P("gx", "gy", "gz", None, None, None),
        P("gx", "gy", "gz", None, None, None),
        P("gx", "gy", "gz", None, None),
        P("gx", "gy", "gz", None, None),
    )
    return jax.shard_map(
        local, mesh=mesh, in_specs=in_specs, out_specs=P(None, "gx", "gy", "gz"), check_vma=False
    )
```

```python
import jax
import jax.numpy as jnp
from jax import lax
from jax.experimental import pallas as pl
from jax.experimental.pallas import tpu as pltpu
from jax.sharding import PartitionSpec as P


PARCEL = 8.0
LATENT = 0.5
TIME_INCREMENT = 0.2
VISCOSITY = 0.5

AXES = ("gx", "gy", "gz")
F32 = jnp.float32
BF16 = jnp.bfloat16
I32 = jnp.int32
FAR_AWAY = -100

OWN = 128
HALO = 64


def swaps(shape):
    nx, ny, nz = shape

    def pairs(target):
        out = []
        for i in range(nx):
            for j in range(ny):
                for k in range(nz):
                    there = target(i, j, k)
                    if there is not None:
                        a, b, c = there
                        out.append(((i * ny + j) * nz + k, (a * ny + b) * nz + c))
        return out

    def d_side(i, j, k):
        if j == 0:
            return (i ^ 1, ny - 1, k)
        if j == ny - 1:
            return (i ^ 1, 0, k)
        return (i, ((j - 1) ^ 1) + 1, k)

    def turn(i, j, k):
        if j in (0, ny - 1):
            return ((i + 2) % nx if i % 2 == 0 else (i - 2) % nx, j, k)
        return None

    return {
        "near": pairs(lambda i, j, k: (i ^ 1, j, k)),
        "far": pairs(lambda i, j, k: ((i - 1) % nx if i % 2 == 0 else (i + 1) % nx, j, k)),
        "turn": pairs(turn),
        "C": pairs(lambda i, j, k: (i, j ^ 1, k)),
        "D": pairs(d_side),
    }


def places():
    i, j = lax.axis_index("gx"), lax.axis_index("gy")
    odd_i, odd_j = lax.rem(i, 2), lax.rem(j, 2)
    wrap = jnp.logical_or(j == 0, j == lax.axis_size("gy") - 1)
    return odd_i, odd_j, wrap


def rows(start, size, unit):
    return pl.ds(pl.multiple_of(start, unit), size)


def post_ends(ref, low, high):
    k, n = lax.axis_index("gz"), ref.shape[0] // 8
    ref[...] = jnp.zeros(ref.shape, F32)
    ref[rows(lax.rem(k + 1, n) * 8, 8, 8), :] = jnp.concatenate(high, axis=0)
    ref[rows(lax.rem(k + n - 1, n) * 8, 8, 8), :] = jnp.concatenate(low, axis=0)


def get_ends(ref):
    k, n = lax.axis_index("gz"), ref.shape[0] // 8
    below = ref[rows(lax.rem(k + n - 1, n) * 8, 8, 8), :]
    above = ref[rows(lax.rem(k + 1, n) * 8, 8, 8), :]
    return below, above


def choose(cond, yes, no):
    pl.when(cond)(yes)
    pl.when(jnp.logical_not(cond))(no)


def pack_y(gas, to_c, to_d):
    _, odd_j, _ = places()

    def put(ref, y):
        for c in range(5):
            ref[c * 8 : c * 8 + 8, :] = gas[pl.ds(c * OWN + y, 8, stride=16), :]

    def even():
        put(to_c, 15)
        put(to_d, 0)

    def odd():
        put(to_c, 0)
        put(to_d, 15)

    choose(odd_j == 0, even, odd)


def pack_x(gas, from_c, from_d, to_near, to_far, to_turn):
    odd_i, _, _ = places()
    near = (1 - odd_i) * 7
    to_near[120:128, :] = jnp.zeros((8, 128), F32)
    to_far[80:96, :] = jnp.zeros((16, 128), F32)
    to_turn[...] = jnp.zeros((8, 128), F32)
    for c in range(5):
        to_near[c * 24 : c * 24 + 16, :] = gas[rows(c * OWN + near * 16, 16, 16), :]
        to_near[c * 24 + 16 : c * 24 + 24, :] = from_d[c * 8 : c * 8 + 8, :]
        to_near[120 + c : 121 + c, :] = from_c[pl.ds(c * 8 + near, 1), :]
        to_far[c * 16 : c * 16 + 16, :] = gas[rows(c * OWN + 112 - near * 16, 16, 16), :]
        to_far[80 + c : 81 + c, :] = from_c[pl.ds(c * 8 + 7 - near, 1), :]
        to_far[88 + c : 89 + c, :] = from_d[pl.ds(c * 8 + 7 - near, 1), :]
        to_turn[c : c + 1, :] = from_d[pl.ds(c * 8 + near, 1), :]


def join_halo(gas, from_c, from_d, from_near, from_far, from_turn, after, halo, ends):
    del after
    odd_i, _, wrap = places()
    near = odd_i * 7
    for c in range(5):
        at = c * HALO
        halo[at : at + 16, :] = from_near[c * 24 : c * 24 + 16, :]
        halo[at + 16 : at + 32, :] = from_far[c * 16 : c * 16 + 16, :]
        halo[at + 32 : at + 40, :] = from_c[c * 8 : c * 8 + 8, :]
        halo[at + 40 : at + 48, :] = jnp.zeros((8, 128), F32)
        halo[at + 40 : at + 41, :] = from_near[120 + c : 121 + c, :]
        halo[at + 41 : at + 42, :] = from_far[80 + c : 81 + c, :]
        halo[at + 56 : at + 64, :] = jnp.zeros((8, 128), F32)
    halo[5 * HALO : 384, :] = jnp.zeros((384 - 5 * HALO, 128), F32)

    def wrapped():
        for c in range(5):
            at = c * HALO + 48
            halo[at : at + 8, :] = from_near[c * 24 + 16 : c * 24 + 24, :]
            halo[at + 8 : at + 9, :] = from_d[pl.ds(c * 8 + near, 1), :]
            halo[at + 9 : at + 10, :] = from_turn[c : c + 1, :]

    def inner():
        for c in range(5):
            at = c * HALO + 48
            halo[at : at + 8, :] = from_d[c * 8 : c * 8 + 8, :]
            halo[at + 8 : at + 9, :] = from_near[pl.ds(c * 24 + 16 + near, 1), :]
            halo[at + 9 : at + 10, :] = from_far[88 + c : 89 + c, :]

    choose(wrap, wrapped, inner)
    turned = []
    for n in range(8):
        part = gas[n * 128 : n * 128 + 128, :] if n < 5 else halo[(n - 5) * 128 : (n - 4) * 128, :]
        turned.append(part.T)
    post_ends(ends, [t[0:1, :] for t in turned], [t[127:128, :] for t in turned])


def three(place, anchor, offset):
    low = 0.5 * (0.5 - offset) * (0.5 - offset)
    middle = 0.75 - offset * offset
    high = 0.5 * (0.5 + offset) * (0.5 + offset)
    step = place - anchor
    return jnp.where(step == -1, low, jnp.where(step == 0, middle, jnp.where(step == 1, high, 0.0)))


def weigh(
    gas, cell, tile, count, frac, mass, vel, temp, after, planar, vertical, across, part, drops
):
    del after
    odd_i, odd_j, _ = places()
    blocks = cell.shape[0]
    drops[0:blocks, :] = jnp.exp(jnp.log(mass[...]) * (1.0 / 3.0))
    slot = lax.broadcasted_iota(I32, (1, 128), 1)
    drops[2 * blocks : 5 * blocks, :] = vel[...]
    drops[5 * blocks : 6 * blocks, :] = temp[...]
    near_x, far_x = 8 - 9 * odd_i, 9 * odd_i - 1
    c_y, d_y = 16 - 17 * odd_j, 17 * odd_j - 1
    r = lax.broadcasted_iota(I32, (192, 128), 0)
    q = r & 15
    group = (r >> 4) - 8
    on_y = jnp.where(q < 8, q, jnp.where(q == 8, near_x, jnp.where(q == 9, far_x, FAR_AWAY)))
    place_x = jnp.where(group < 0, r >> 4, jnp.where(group == 0, near_x, jnp.where(group == 1, far_x, on_y)))
    place_y = jnp.where(group == 2, c_y, jnp.where(group == 3, d_y, q))
    s = lax.broadcasted_iota(I32, (256, 128), 0)
    place_z = jnp.where(s < 128, s, jnp.where(s == 128, -1, jnp.where(s == 129, 128, FAR_AWAY)))
    cells = gas[...].astype(BF16)
    for b in range(blocks):
        lanes = slice(b * 128, b * 128 + 128)
        at = cell[b : b + 1, :]
        wx = three(place_x, at >> 10, frac[b : b + 1, :])
        drops[blocks + b : blocks + b + 1, :] = jnp.where(slot < count[0:1, b : b + 1], PARCEL, 0.0).astype(F32)
        wy = three(place_y, ((at >> 7) & 7) + 8 * tile[0:1, b : b + 1], frac[blocks + b : blocks + b + 1, :])
        wz = three(place_z, at & 127, frac[2 * blocks + b : 2 * blocks + b + 1, :])
        flat = (wx * wy).astype(BF16)
        planar[0:192, lanes] = flat
        planar[192:256, lanes] = jnp.zeros((64, 128), BF16)
        vertical[:, lanes] = wz[0:144, :].astype(BF16)
        across[lanes, :] = jnp.concatenate([wz[0:128, :].T, wz[128:256, :].T], axis=1).astype(BF16)
        seen = jnp.dot(cells, wz[0:128, :].astype(BF16), preferred_element_type=F32)
        own = flat[0:128, :].astype(F32)
        for c in range(5):
            part[c * blocks + b : c * blocks + b + 1, :] = jnp.sum(
                seen[c * OWN : c * OWN + OWN, :] * own, axis=0, keepdims=True
            )


def deposit(halo, z_ends, planar, vertical, across, part, drops, sums, ghosts, gas_at, source, weighted):
    blocks = drops.shape[0] // 6
    below, above = get_ends(z_ends)

    def z_rows(v):
        turned = pltpu.roll(v, 64, 1)
        side = jnp.concatenate(
            [v[5:6], turned[5:6], v[6:7], turned[6:7], v[7:8], jnp.zeros((3, 128), F32)], axis=0
        )
        return jnp.concatenate([v, side], axis=1)

    ends = jnp.concatenate([z_rows(below), z_rows(above)], axis=0).astype(BF16)
    at_ends = jnp.dot(ends, planar[...], preferred_element_type=F32)
    around = halo[0 : 5 * HALO, :].astype(BF16)
    for b in range(0, blocks, 2):
        lanes = slice(b * 128, b * 128 + 256)
        seen = jnp.dot(around, vertical[0:128, lanes], preferred_element_type=F32)
        side = planar[128:192, lanes].astype(F32)
        edge = vertical[128:144, lanes].astype(F32)
        ended = at_ends[0:8, lanes] * edge[0:1, :] + at_ends[8:16, lanes] * edge[1:2, :]
        for c in range(5):
            n = c * blocks + b
            row = ended[c : c + 1, :] + jnp.sum(seen[c * HALO : c * HALO + HALO, :] * side, axis=0, keepdims=True)
            gas_at[n : n + 1, :] = part[n : n + 1, :] + row[:, 0:128]
            gas_at[n + 1 : n + 2, :] = part[n + 1 : n + 2, :] + row[:, 128:256]
    d = drops[0:blocks, :]
    live = drops[blocks : 2 * blocks, :]
    warm = gas_at[4 * blocks : 5 * blocks, :] - drops[5 * blocks : 6 * blocks, :]
    soft = jnp.maximum(warm, 0.0) + jnp.log1p(jnp.exp(-jnp.abs(warm)))
    rate = d * jnp.log1p(soft)
    pull = d * gas_at[0:blocks, :]
    source[0:blocks, :] = rate * live
    for m in range(1, 4):
        v = drops[(m + 1) * blocks : (m + 2) * blocks, :]
        u = gas_at[m * blocks : (m + 1) * blocks, :]
        source[m * blocks : (m + 1) * blocks, :] = (rate * v - pull * (u - v)) * live
    source[4 * blocks : 5 * blocks, :] = (-(d * warm) - LATENT * rate) * live
    for b in range(blocks):
        lanes = slice(b * 128, b * 128 + 128)
        flat = planar[0:192, lanes].astype(F32)
        for c in range(5):
            scaled = (flat * source[c * blocks + b : c * blocks + b + 1, :]).astype(BF16)
            weighted[c * OWN : c * OWN + OWN, lanes] = scaled[0:128, :]
            weighted[640 + c * HALO : 640 + c * HALO + HALO, lanes] = scaled[128:192, :]
    low, high = [], []
    for n in range(8):
        size = 128 if n < 7 else 64
        total = jnp.dot(weighted[n * 128 : n * 128 + size, :], across[...], preferred_element_type=F32)
        sums[n * 128 : n * 128 + size, :] = total[:, 0:128]
        ends = total[:, 128:256]
        if size < 128:
            ends = jnp.concatenate([ends, jnp.zeros((128 - size, 128), F32)], axis=0)
        turned = ends.T
        low.append(turned[0:1, :])
        high.append(turned[1:2, :])
    post_ends(ghosts, low, high)


def upright(below, above):
    z = lax.broadcasted_iota(I32, (128, 128), 0)
    return jnp.where(z == 0, below, jnp.where(z == 127, above, 0.0)).T


def fold_z(sums, z_ends, own, sides, to_c, to_d):
    below, above = get_ends(z_ends)
    for n in range(8):
        extra = upright(below[n : n + 1, :], above[n : n + 1, :])
        if n < 5:
            own[n * OWN : n * OWN + OWN, :] = sums[n * OWN : n * OWN + OWN, :] + extra
            continue
        for half in range(2):
            c = (n - 5) * 2 + half
            if c > 4:
                continue
            at = 640 + c * HALO
            here = sums[at : at + HALO, :] + extra[half * 64 : half * 64 + 64, :]
            sides[c * 32 : c * 32 + 32, :] = here[0:32, :]
            to_c[c * 16 : c * 16 + 16, :] = here[32:48, :]
            to_d[c * 16 : c * 16 + 16, :] = here[48:64, :]


def fold_y(sides, from_c, from_d, to_near, to_far, to_turn):
    _, odd_j, wrap = places()
    keep = jnp.where(wrap, 0.0, 1.0).astype(F32)
    y = lax.broadcasted_iota(I32, (16, 128), 0)
    c_y = 15 - 15 * odd_j
    at_c, at_d = y == c_y, y == 15 - c_y
    to_turn[...] = jnp.zeros((8, 128), F32)
    for c in range(5):
        for side in range(2):
            row = c * 16 + 8 + side
            folded = (
                sides[c * 32 + side * 16 : c * 32 + side * 16 + 16, :]
                + jnp.where(at_c, from_c[row : row + 1, :], 0.0)
                + jnp.where(at_d, from_d[row : row + 1, :] * keep, 0.0)
            )
            if side == 0:
                to_near[c * 24 : c * 24 + 16, :] = folded
            else:
                to_far[c * 16 : c * 16 + 16, :] = folded
        to_near[c * 24 + 16 : c * 24 + 24, :] = from_d[c * 16 : c * 16 + 8, :]
        to_turn[c : c + 1, :] = from_d[c * 16 + 9 : c * 16 + 10, :]


def stencil(gas, start, halo, z_ends, own, from_c, from_d, after, out, upper):
    del after
    below, above = get_ends(z_ends)
    odd_i, odd_j, wrap = places()
    keep = jnp.where(wrap, 0.0, 1.0).astype(F32)
    y = lax.broadcasted_iota(I32, (16, 128), 0)
    z = lax.broadcasted_iota(I32, (16, 128), 1)
    c_y = 15 - 15 * odd_j
    at_c, at_d = y == c_y, y == 15 - c_y
    near = (1 - odd_i) * 7
    high_x, low_x = 16 * odd_i, 16 - 16 * odd_i
    high_y, low_y = 32 + 16 * odd_j, 48 - 16 * odd_j
    for c in range(5):
        upper[...] = upright(below[c : c + 1, :], above[c : c + 1, :])
        for x in range(8):
            at = c * OWN + x * 16
            g = gas[at : at + 16, :]
            if x < 7:
                x_up = gas[at + 16 : at + 32, :]
            else:
                x_up = halo[rows(c * HALO + high_x, 16, 16), :]
            if x > 0:
                x_down = gas[at - 16 : at, :]
            else:
                x_down = halo[rows(c * HALO + low_x, 16, 16), :]
            y_up = jnp.where(y == 15, halo[pl.ds(c * HALO + high_y + x, 1), :], pltpu.roll(g, 15, 0))
            y_down = jnp.where(y == 0, halo[pl.ds(c * HALO + low_y + x, 1), :], pltpu.roll(g, 1, 0))
            ends = upper[x * 16 : x * 16 + 16, :]
            z_up = jnp.where(z == 127, ends, pltpu.roll(g, 127, 1))
            z_down = jnp.where(z == 0, ends, pltpu.roll(g, 1, 1))
            laplace = -6.0 * g + (x_up + x_down) + (y_up + y_down) + (z_up + z_down)
            advect = 0.5 * (
                gas[OWN + x * 16 : OWN + x * 16 + 16, :] * (x_up - x_down)
                + gas[2 * OWN + x * 16 : 2 * OWN + x * 16 + 16, :] * (y_up - y_down)
                + gas[3 * OWN + x * 16 : 3 * OWN + x * 16 + 16, :] * (z_up - z_down)
            )
            across = jnp.where(wrap & (near == x), 1.0, 0.0).astype(F32)
            added = (
                own[at : at + 16, :]
                + jnp.where(at_c, from_c[c * 16 + x : c * 16 + x + 1, :], 0.0)
                + jnp.where(
                    at_d,
                    from_d[c * 16 + x : c * 16 + x + 1, :] * keep + from_d[c * 16 + 8 : c * 16 + 9, :] * across,
                    0.0,
                )
            )
            out[at : at + 16, :] = 0.75 * start[at : at + 16, :] + 0.25 * (
                g + TIME_INCREMENT * (VISCOSITY * laplace - advect + added)
            )


def finish(base, from_near, from_far, from_turn, out):
    odd_i, odd_j, wrap = places()
    near = (1 - odd_i) * 112
    scale = 0.25 * TIME_INCREMENT
    gate = jnp.where(wrap, scale, 0.0).astype(F32)
    at_d = lax.broadcasted_iota(I32, (16, 128), 0) == 15 * odd_j
    out[...] = base[...]
    for c in range(5):
        at = rows(c * OWN + near, 16, 16)
        out[at, :] = out[at, :] + scale * from_near[c * 24 : c * 24 + 16, :]
        at = rows(c * OWN + 112 - near, 16, 16)
        turned = jnp.where(at_d, from_turn[c : c + 1, :] * gate, 0.0)
        out[at, :] = out[at, :] + scale * from_far[c * 16 : c * 16 + 16, :] + turned

    def across(y):
        def add():
            for c in range(5):
                at = pl.ds(c * OWN + y, 8, stride=16)
                out[at, :] = out[at, :] + scale * from_near[c * 24 + 16 : c * 24 + 24, :]

        return add

    pl.when(wrap & (odd_j == 0))(across(0))
    pl.when(wrap & (odd_j == 1))(across(15))


def call(body, out_shapes, *operands, loose=(), scratch=(), flops=10000):
    whole = pl.BlockSpec(memory_space=pltpu.VMEM)
    anywhere = pl.BlockSpec(memory_space=pl.ANY)
    single = not isinstance(out_shapes, list)
    outs = [out_shapes] if single else out_shapes
    result = pl.pallas_call(
        body,
        out_shape=[jax.ShapeDtypeStruct(s, t) for s, t in outs],
        in_specs=[anywhere if n in loose else whole for n in range(len(operands))],
        out_specs=[whole] * len(outs),
        scratch_shapes=list(scratch),
        compiler_params=pltpu.CompilerParams(vmem_limit_bytes=24 * 1024 * 1024),
        cost_estimate=pl.CostEstimate(flops=flops, bytes_accessed=100000, transcendentals=0),
    )(*operands)
    return result[0] if single else result


def local(gas_state, section_start, drop_cell, block_tile, droplets_per_block, drop_frac, drop_vel, drop_mass, drop_temp):
    shape = tuple(lax.axis_size(a) for a in AXES)
    routes = swaps(shape)

    def send(values, route):
        return lax.ppermute(values, AXES, routes[route])

    def swap_ends(values):
        chunks = values.reshape(shape[2], 8, 128)
        return lax.all_to_all(chunks, "gz", 0, 0).reshape(values.shape)

    blocks = drop_cell.shape[3]
    ends_shape = ((8 * shape[2], 128), F32)
    gas = gas_state.reshape(640, 128)
    start = section_start.reshape(640, 128)
    cell = drop_cell.reshape(blocks, 128)
    frac = drop_frac.reshape(3 * blocks, 128)
    vel = drop_vel.reshape(3 * blocks, 128)
    temp = drop_temp.reshape(blocks, 128)
    mass = drop_mass.reshape(blocks, 128)
    count = droplets_per_block.reshape(1, blocks)
    tile = block_tile.reshape(1, blocks)

    to_c, to_d = call(pack_y, [((40, 128), F32)] * 2, gas)
    gas_d, gas_c = send(to_d, "D"), send(to_c, "C")
    to_near, to_far, to_turn = call(pack_x, [((128, 128), F32), ((96, 128), F32), ((8, 128), F32)], gas, gas_c, gas_d)
    gas_near, gas_far = send(to_near, "near"), send(to_far, "far")
    gas_turn = send(to_turn, "turn")
    planar, vertical, across, part, drops = call(
        weigh,
        [
            ((256, blocks * 128), BF16),
            ((144, blocks * 128), BF16),
            ((blocks * 128, 256), BF16),
            ((5 * blocks, 128), F32),
            ((6 * blocks, 128), F32),
        ],
        gas, cell, tile, count, frac, mass, vel, temp, to_near,
        loose=(8,), flops=1 << 32,
    )
    halo, ends = call(
        join_halo, [((384, 128), F32), ends_shape],
        gas, gas_c, gas_d, gas_near, gas_far, gas_turn, part,
        loose=(6,),
    )
    ends = swap_ends(ends)
    sums, ghosts = call(
        deposit, [((960, 128), F32), ends_shape],
        halo, ends, planar, vertical, across, part, drops,
        scratch=[
            pltpu.VMEM((5 * blocks, 128), F32),
            pltpu.VMEM((5 * blocks, 128), F32),
            pltpu.VMEM((960, blocks * 128), BF16),
        ],
    )
    own, sides, to_c, to_d = call(
        fold_z, [((640, 128), F32), ((160, 128), F32), ((80, 128), F32), ((80, 128), F32)],
        sums, swap_ends(ghosts),
    )
    dep_d, dep_c = send(to_d, "D"), send(to_c, "C")
    to_near, to_far, to_turn = call(fold_y, [((120, 128), F32), ((80, 128), F32), ((8, 128), F32)], sides, dep_c, dep_d)
    dep_near, dep_far = send(to_near, "near"), send(to_far, "far")
    dep_turn = send(to_turn, "turn")
    base = call(
        stencil, ((640, 128), F32),
        gas, start, halo, ends, own, dep_c, dep_d, to_near,
        loose=(7,), scratch=[pltpu.VMEM((128, 128), F32)], flops=1 << 32,
    )
    out = call(finish, ((640, 128), F32), base, dep_near, dep_far, dep_turn)
    return out.reshape(gas_state.shape)


def solution(mesh):
    in_specs = (
        P(None, "gx", "gy", "gz"),
        P(None, "gx", "gy", "gz"),
        P("gx", "gy", "gz", None, None),
        P("gx", "gy", "gz", None),
        P("gx", "gy", "gz", None),
        P("gx", "gy", "gz", None, None, None),
        P("gx", "gy", "gz", None, None, None),
        P("gx", "gy", "gz", None, None),
        P("gx", "gy", "gz", None, None),
    )
    return jax.shard_map(
        local, mesh=mesh, in_specs=in_specs, out_specs=P(None, "gx", "gy", "gz"), check_vma=False
    )
```

```python
import jax
import jax.numpy as jnp
from jax import lax
from jax.experimental import pallas as pl
from jax.experimental.pallas import tpu as pltpu
from jax.sharding import PartitionSpec as P


PARCEL = 8.0
LATENT = 0.5
TIME_INCREMENT = 0.2
VISCOSITY = 0.5

AXES = ("gx", "gy", "gz")
F32 = jnp.float32
BF16 = jnp.bfloat16
I32 = jnp.int32
FAR_AWAY = -100

OWN = 128
HALO = 64


def swaps(shape):
    nx, ny, nz = shape

    def pairs(target):
        out = []
        for i in range(nx):
            for j in range(ny):
                for k in range(nz):
                    there = target(i, j, k)
                    if there is not None:
                        a, b, c = there
                        out.append(((i * ny + j) * nz + k, (a * ny + b) * nz + c))
        return out

    def d_side(i, j, k):
        if j == 0:
            return (i ^ 1, ny - 1, k)
        if j == ny - 1:
            return (i ^ 1, 0, k)
        return (i, ((j - 1) ^ 1) + 1, k)

    def turn(i, j, k):
        if j in (0, ny - 1):
            return ((i + 2) % nx if i % 2 == 0 else (i - 2) % nx, j, k)
        return None

    return {
        "near": pairs(lambda i, j, k: (i ^ 1, j, k) if 0 < j < ny - 1 else None),
        "carry": pairs(lambda i, j, k: (i ^ 1, j, k) if j in (0, ny - 1) else None),
        "far": pairs(lambda i, j, k: ((i - 1) % nx if i % 2 == 0 else (i + 1) % nx, j, k)),
        "turn": pairs(turn),
        "C": pairs(lambda i, j, k: (i, j ^ 1, k)),
        "D": pairs(d_side),
    }


def places():
    i, j = lax.axis_index("gx"), lax.axis_index("gy")
    odd_i, odd_j = lax.rem(i, 2), lax.rem(j, 2)
    wrap = jnp.logical_or(j == 0, j == lax.axis_size("gy") - 1)
    return odd_i, odd_j, wrap


def rows(start, size, unit):
    return pl.ds(pl.multiple_of(start, unit), size)


def post_ends(ref, low, high):
    k, n = lax.axis_index("gz"), ref.shape[0] // 8
    ref[...] = jnp.zeros(ref.shape, F32)
    ref[rows(lax.rem(k + 1, n) * 8, 8, 8), :] = jnp.concatenate(high, axis=0)
    ref[rows(lax.rem(k + n - 1, n) * 8, 8, 8), :] = jnp.concatenate(low, axis=0)


def get_ends(ref):
    k, n = lax.axis_index("gz"), ref.shape[0] // 8
    below = ref[rows(lax.rem(k + n - 1, n) * 8, 8, 8), :]
    above = ref[rows(lax.rem(k + 1, n) * 8, 8, 8), :]
    return below, above


def choose(cond, yes, no):
    pl.when(cond)(yes)
    pl.when(jnp.logical_not(cond))(no)


def pack_y(gas, to_c, to_d):
    _, odd_j, _ = places()

    def put(ref, y):
        for c in range(5):
            ref[c * 8 : c * 8 + 8, :] = gas[pl.ds(c * OWN + y, 8, stride=16), :]

    def even():
        put(to_c, 15)
        put(to_d, 0)

    def odd():
        put(to_c, 0)
        put(to_d, 15)

    choose(odd_j == 0, even, odd)


def pack_x(gas, from_c, from_d, to_near, to_carry, to_far, to_turn):
    odd_i, _, _ = places()
    near = (1 - odd_i) * 7
    to_turn[...] = jnp.zeros((8, 128), F32)
    to_far[80:96, :] = jnp.zeros((16, 128), F32)
    for c in range(5):
        to_far[c * 16 : c * 16 + 16, :] = gas[rows(c * OWN + 112 - near * 16, 16, 16), :]
        to_far[80 + c : 81 + c, :] = from_c[pl.ds(c * 8 + 7 - near, 1), :]
        to_far[88 + c : 89 + c, :] = from_d[pl.ds(c * 8 + 7 - near, 1), :]
        to_turn[c : c + 1, :] = from_d[pl.ds(c * 8 + near, 1), :]
    to_near[80:96, :] = jnp.zeros((16, 128), F32)
    to_carry[120:128, :] = jnp.zeros((8, 128), F32)
    for c in range(5):
        face = gas[rows(c * OWN + near * 16, 16, 16), :]
        to_near[c * 16 : c * 16 + 16, :] = face
        to_near[80 + c : 81 + c, :] = from_c[pl.ds(c * 8 + near, 1), :]
        to_near[88 + c : 89 + c, :] = from_d[pl.ds(c * 8 + near, 1), :]
        to_carry[c * 24 : c * 24 + 16, :] = face
        to_carry[c * 24 + 16 : c * 24 + 24, :] = from_d[c * 8 : c * 8 + 8, :]
        to_carry[120 + c : 121 + c, :] = from_c[pl.ds(c * 8 + near, 1), :]


def join_halo(gas, from_c, from_d, from_near, from_carry, from_far, from_turn, after, halo, ends):
    del after
    odd_i, _, wrap = places()
    near = odd_i * 7
    for c in range(5):
        at = c * HALO
        halo[at + 16 : at + 32, :] = from_far[c * 16 : c * 16 + 16, :]
        halo[at + 32 : at + 40, :] = from_c[c * 8 : c * 8 + 8, :]
        halo[at + 40 : at + 48, :] = jnp.zeros((8, 128), F32)
        halo[at + 41 : at + 42, :] = from_far[80 + c : 81 + c, :]
        halo[at + 56 : at + 64, :] = jnp.zeros((8, 128), F32)
    halo[5 * HALO : 384, :] = jnp.zeros((384 - 5 * HALO, 128), F32)

    def wrapped():
        for c in range(5):
            at = c * HALO
            halo[at : at + 16, :] = from_carry[c * 24 : c * 24 + 16, :]
            halo[at + 40 : at + 41, :] = from_carry[120 + c : 121 + c, :]
            halo[at + 48 : at + 56, :] = from_carry[c * 24 + 16 : c * 24 + 24, :]
            halo[at + 56 : at + 57, :] = from_d[pl.ds(c * 8 + near, 1), :]
            halo[at + 57 : at + 58, :] = from_turn[c : c + 1, :]

    def inner():
        for c in range(5):
            at = c * HALO
            halo[at : at + 16, :] = from_near[c * 16 : c * 16 + 16, :]
            halo[at + 40 : at + 41, :] = from_near[80 + c : 81 + c, :]
            halo[at + 48 : at + 56, :] = from_d[c * 8 : c * 8 + 8, :]
            halo[at + 56 : at + 57, :] = from_near[88 + c : 89 + c, :]
            halo[at + 57 : at + 58, :] = from_far[88 + c : 89 + c, :]

    choose(wrap, wrapped, inner)
    turned = []
    for n in range(8):
        part = gas[n * 128 : n * 128 + 128, :] if n < 5 else halo[(n - 5) * 128 : (n - 4) * 128, :]
        turned.append(part.T)
    post_ends(ends, [t[0:1, :] for t in turned], [t[127:128, :] for t in turned])


def three(place, anchor, offset):
    low = 0.5 * (0.5 - offset) * (0.5 - offset)
    middle = 0.75 - offset * offset
    high = 0.5 * (0.5 + offset) * (0.5 + offset)
    step = place - anchor
    return jnp.where(step == -1, low, jnp.where(step == 0, middle, jnp.where(step == 1, high, 0.0)))


def weigh(
    gas, cell, tile, count, frac, mass, vel, temp, after, planar, vertical, across, part, drops
):
    del after
    odd_i, odd_j, _ = places()
    blocks = cell.shape[0]
    drops[0:blocks, :] = jnp.exp(jnp.log(mass[...]) * (1.0 / 3.0))
    slot = lax.broadcasted_iota(I32, (1, 128), 1)
    drops[2 * blocks : 5 * blocks, :] = vel[...]
    drops[5 * blocks : 6 * blocks, :] = temp[...]
    near_x, far_x = 8 - 9 * odd_i, 9 * odd_i - 1
    c_y, d_y = 16 - 17 * odd_j, 17 * odd_j - 1
    r = lax.broadcasted_iota(I32, (192, 128), 0)
    q = r & 15
    group = (r >> 4) - 8
    on_y = jnp.where(q < 8, q, jnp.where(q == 8, near_x, jnp.where(q == 9, far_x, FAR_AWAY)))
    place_x = jnp.where(group < 0, r >> 4, jnp.where(group == 0, near_x, jnp.where(group == 1, far_x, on_y)))
    place_y = jnp.where(group == 2, c_y, jnp.where(group == 3, d_y, q))
    s = lax.broadcasted_iota(I32, (256, 128), 0)
    place_z = jnp.where(s < 128, s, jnp.where(s == 128, -1, jnp.where(s == 129, 128, FAR_AWAY)))
    cells = gas[...].astype(BF16)
    for b in range(blocks):
        lanes = slice(b * 128, b * 128 + 128)
        at = cell[b : b + 1, :]
        wx = three(place_x, at >> 10, frac[b : b + 1, :])
        drops[blocks + b : blocks + b + 1, :] = jnp.where(slot < count[0:1, b : b + 1], PARCEL, 0.0).astype(F32)
        wy = three(place_y, ((at >> 7) & 7) + 8 * tile[0:1, b : b + 1], frac[blocks + b : blocks + b + 1, :])
        wz = three(place_z, at & 127, frac[2 * blocks + b : 2 * blocks + b + 1, :])
        flat = (wx * wy).astype(BF16)
        planar[0:192, lanes] = flat
        planar[192:256, lanes] = jnp.zeros((64, 128), BF16)
        vertical[:, lanes] = wz[0:144, :].astype(BF16)
        across[lanes, :] = jnp.concatenate([wz[0:128, :].T, wz[128:256, :].T], axis=1).astype(BF16)
        seen = jnp.dot(cells, wz[0:128, :].astype(BF16), preferred_element_type=F32)
        own = flat[0:128, :].astype(F32)
        for c in range(5):
            part[c * blocks + b : c * blocks + b + 1, :] = jnp.sum(
                seen[c * OWN : c * OWN + OWN, :] * own, axis=0, keepdims=True
            )


def deposit(halo, z_ends, planar, vertical, across, part, drops, sums, ghosts, gas_at, source, weighted):
    blocks = drops.shape[0] // 6
    below, above = get_ends(z_ends)

    def z_rows(v):
        turned = pltpu.roll(v, 64, 1)
        side = jnp.concatenate(
            [v[5:6], turned[5:6], v[6:7], turned[6:7], v[7:8], jnp.zeros((3, 128), F32)], axis=0
        )
        return jnp.concatenate([v, side], axis=1)

    ends = jnp.concatenate([z_rows(below), z_rows(above)], axis=0).astype(BF16)
    at_ends = jnp.dot(ends, planar[...], preferred_element_type=F32)
    around = halo[0 : 5 * HALO, :].astype(BF16)
    for b in range(0, blocks, 2):
        lanes = slice(b * 128, b * 128 + 256)
        seen = jnp.dot(around, vertical[0:128, lanes], preferred_element_type=F32)
        side = planar[128:192, lanes].astype(F32)
        edge = vertical[128:144, lanes].astype(F32)
        ended = at_ends[0:8, lanes] * edge[0:1, :] + at_ends[8:16, lanes] * edge[1:2, :]
        for c in range(5):
            n = c * blocks + b
            row = ended[c : c + 1, :] + jnp.sum(seen[c * HALO : c * HALO + HALO, :] * side, axis=0, keepdims=True)
            gas_at[n : n + 1, :] = part[n : n + 1, :] + row[:, 0:128]
            gas_at[n + 1 : n + 2, :] = part[n + 1 : n + 2, :] + row[:, 128:256]
    d = drops[0:blocks, :]
    live = drops[blocks : 2 * blocks, :]
    warm = gas_at[4 * blocks : 5 * blocks, :] - drops[5 * blocks : 6 * blocks, :]
    soft = jnp.maximum(warm, 0.0) + jnp.log1p(jnp.exp(-jnp.abs(warm)))
    rate = d * jnp.log1p(soft)
    pull = d * gas_at[0:blocks, :]
    source[0:blocks, :] = rate * live
    for m in range(1, 4):
        v = drops[(m + 1) * blocks : (m + 2) * blocks, :]
        u = gas_at[m * blocks : (m + 1) * blocks, :]
        source[m * blocks : (m + 1) * blocks, :] = (rate * v - pull * (u - v)) * live
    source[4 * blocks : 5 * blocks, :] = (-(d * warm) - LATENT * rate) * live
    for b in range(blocks):
        lanes = slice(b * 128, b * 128 + 128)
        flat = planar[0:192, lanes].astype(F32)
        for c in range(5):
            scaled = (flat * source[c * blocks + b : c * blocks + b + 1, :]).astype(BF16)
            weighted[c * OWN : c * OWN + OWN, lanes] = scaled[0:128, :]
            weighted[640 + c * HALO : 640 + c * HALO + HALO, lanes] = scaled[128:192, :]
    low, high = [], []
    for n in range(8):
        size = 128 if n < 7 else 64
        total = jnp.dot(weighted[n * 128 : n * 128 + size, :], across[...], preferred_element_type=F32)
        sums[n * 128 : n * 128 + size, :] = total[:, 0:128]
        ends = total[:, 128:256]
        if size < 128:
            ends = jnp.concatenate([ends, jnp.zeros((128 - size, 128), F32)], axis=0)
        turned = ends.T
        low.append(turned[0:1, :])
        high.append(turned[1:2, :])
    post_ends(ghosts, low, high)


def upright(below, above):
    z = lax.broadcasted_iota(I32, (128, 128), 0)
    return jnp.where(z == 0, below, jnp.where(z == 127, above, 0.0)).T


def fold_z(sums, z_ends, own, sides, to_c, to_d):
    below, above = get_ends(z_ends)
    for n in range(8):
        extra = upright(below[n : n + 1, :], above[n : n + 1, :])
        if n < 5:
            own[n * OWN : n * OWN + OWN, :] = sums[n * OWN : n * OWN + OWN, :] + extra
            continue
        for half in range(2):
            c = (n - 5) * 2 + half
            if c > 4:
                continue
            at = 640 + c * HALO
            here = sums[at : at + HALO, :] + extra[half * 64 : half * 64 + 64, :]
            sides[c * 32 : c * 32 + 32, :] = here[0:32, :]
            to_c[c * 16 : c * 16 + 16, :] = here[32:48, :]
            to_d[c * 16 : c * 16 + 16, :] = here[48:64, :]


def fold_y(sides, from_c, from_d, to_near, to_carry, to_far, to_turn):
    _, odd_j, wrap = places()
    keep = jnp.where(wrap, 0.0, 1.0).astype(F32)
    y = lax.broadcasted_iota(I32, (16, 128), 0)
    c_y = 15 - 15 * odd_j
    at_c, at_d = y == c_y, y == 15 - c_y
    to_turn[...] = jnp.zeros((8, 128), F32)
    for c in range(5):
        for side in range(2):
            row = c * 16 + 8 + side
            folded = (
                sides[c * 32 + side * 16 : c * 32 + side * 16 + 16, :]
                + jnp.where(at_c, from_c[row : row + 1, :], 0.0)
                + jnp.where(at_d, from_d[row : row + 1, :] * keep, 0.0)
            )
            if side == 0:
                to_near[c * 16 : c * 16 + 16, :] = folded
                to_carry[c * 24 : c * 24 + 16, :] = folded
            else:
                to_far[c * 16 : c * 16 + 16, :] = folded
        to_carry[c * 24 + 16 : c * 24 + 24, :] = from_d[c * 16 : c * 16 + 8, :]
        to_turn[c : c + 1, :] = from_d[c * 16 + 9 : c * 16 + 10, :]


def stencil(gas, start, halo, z_ends, own, from_c, from_d, after, out, upper):
    del after
    below, above = get_ends(z_ends)
    odd_i, odd_j, wrap = places()
    keep = jnp.where(wrap, 0.0, 1.0).astype(F32)
    y = lax.broadcasted_iota(I32, (16, 128), 0)
    z = lax.broadcasted_iota(I32, (16, 128), 1)
    c_y = 15 - 15 * odd_j
    at_c, at_d = y == c_y, y == 15 - c_y
    near = (1 - odd_i) * 7
    high_x, low_x = 16 * odd_i, 16 - 16 * odd_i
    high_y, low_y = 32 + 16 * odd_j, 48 - 16 * odd_j
    for c in range(5):
        upper[...] = upright(below[c : c + 1, :], above[c : c + 1, :])
        for x in range(8):
            at = c * OWN + x * 16
            g = gas[at : at + 16, :]
            if x < 7:
                x_up = gas[at + 16 : at + 32, :]
            else:
                x_up = halo[rows(c * HALO + high_x, 16, 16), :]
            if x > 0:
                x_down = gas[at - 16 : at, :]
            else:
                x_down = halo[rows(c * HALO + low_x, 16, 16), :]
            y_up = jnp.where(y == 15, halo[pl.ds(c * HALO + high_y + x, 1), :], pltpu.roll(g, 15, 0))
            y_down = jnp.where(y == 0, halo[pl.ds(c * HALO + low_y + x, 1), :], pltpu.roll(g, 1, 0))
            ends = upper[x * 16 : x * 16 + 16, :]
            z_up = jnp.where(z == 127, ends, pltpu.roll(g, 127, 1))
            z_down = jnp.where(z == 0, ends, pltpu.roll(g, 1, 1))
            laplace = -6.0 * g + (x_up + x_down) + (y_up + y_down) + (z_up + z_down)
            advect = 0.5 * (
                gas[OWN + x * 16 : OWN + x * 16 + 16, :] * (x_up - x_down)
                + gas[2 * OWN + x * 16 : 2 * OWN + x * 16 + 16, :] * (y_up - y_down)
                + gas[3 * OWN + x * 16 : 3 * OWN + x * 16 + 16, :] * (z_up - z_down)
            )
            across = jnp.where(wrap & (near == x), 1.0, 0.0).astype(F32)
            added = (
                own[at : at + 16, :]
                + jnp.where(at_c, from_c[c * 16 + x : c * 16 + x + 1, :], 0.0)
                + jnp.where(
                    at_d,
                    from_d[c * 16 + x : c * 16 + x + 1, :] * keep + from_d[c * 16 + 8 : c * 16 + 9, :] * across,
                    0.0,
                )
            )
            out[at : at + 16, :] = 0.75 * start[at : at + 16, :] + 0.25 * (
                g + TIME_INCREMENT * (VISCOSITY * laplace - advect + added)
            )


def finish(base, from_near, from_carry, from_far, from_turn, out):
    odd_i, odd_j, wrap = places()
    near = (1 - odd_i) * 112
    scale = 0.25 * TIME_INCREMENT
    gate = jnp.where(wrap, scale, 0.0).astype(F32)
    at_d = lax.broadcasted_iota(I32, (16, 128), 0) == 15 * odd_j
    out[...] = base[...]
    for c in range(5):
        at = rows(c * OWN + near, 16, 16)
        out[at, :] = out[at, :] + scale * (
            from_near[c * 16 : c * 16 + 16, :] + from_carry[c * 24 : c * 24 + 16, :]
        )
        at = rows(c * OWN + 112 - near, 16, 16)
        turned = jnp.where(at_d, from_turn[c : c + 1, :] * gate, 0.0)
        out[at, :] = out[at, :] + scale * from_far[c * 16 : c * 16 + 16, :] + turned

    def across(y):
        def add():
            for c in range(5):
                at = pl.ds(c * OWN + y, 8, stride=16)
                out[at, :] = out[at, :] + scale * from_carry[c * 24 + 16 : c * 24 + 24, :]

        return add

    pl.when(wrap & (odd_j == 0))(across(0))
    pl.when(wrap & (odd_j == 1))(across(15))


def call(body, out_shapes, *operands, loose=(), scratch=(), flops=10000):
    whole = pl.BlockSpec(memory_space=pltpu.VMEM)
    anywhere = pl.BlockSpec(memory_space=pl.ANY)
    single = not isinstance(out_shapes, list)
    outs = [out_shapes] if single else out_shapes
    result = pl.pallas_call(
        body,
        out_shape=[jax.ShapeDtypeStruct(s, t) for s, t in outs],
        in_specs=[anywhere if n in loose else whole for n in range(len(operands))],
        out_specs=[whole] * len(outs),
        scratch_shapes=list(scratch),
        compiler_params=pltpu.CompilerParams(vmem_limit_bytes=24 * 1024 * 1024),
        cost_estimate=pl.CostEstimate(flops=flops, bytes_accessed=100000, transcendentals=0),
    )(*operands)
    return result[0] if single else result


def local(gas_state, section_start, drop_cell, block_tile, droplets_per_block, drop_frac, drop_vel, drop_mass, drop_temp):
    shape = tuple(lax.axis_size(a) for a in AXES)
    routes = swaps(shape)

    def send(values, route):
        return lax.ppermute(values, AXES, routes[route])

    def swap_ends(values):
        chunks = values.reshape(shape[2], 8, 128)
        return lax.all_to_all(chunks, "gz", 0, 0).reshape(values.shape)

    blocks = drop_cell.shape[3]
    ends_shape = ((8 * shape[2], 128), F32)
    gas = gas_state.reshape(640, 128)
    start = section_start.reshape(640, 128)
    cell = drop_cell.reshape(blocks, 128)
    frac = drop_frac.reshape(3 * blocks, 128)
    vel = drop_vel.reshape(3 * blocks, 128)
    temp = drop_temp.reshape(blocks, 128)
    mass = drop_mass.reshape(blocks, 128)
    count = droplets_per_block.reshape(1, blocks)
    tile = block_tile.reshape(1, blocks)

    to_c, to_d = call(pack_y, [((40, 128), F32)] * 2, gas)
    gas_d, gas_c = send(to_d, "D"), send(to_c, "C")
    to_near, to_carry, to_far, to_turn = call(
        pack_x, [((96, 128), F32), ((128, 128), F32), ((96, 128), F32), ((8, 128), F32)],
        gas, gas_c, gas_d,
    )
    gas_near, gas_far = send(to_near, "near"), send(to_far, "far")
    gas_carry = send(to_carry, "carry")
    gas_turn = send(to_turn, "turn")
    planar, vertical, across, part, drops = call(
        weigh,
        [
            ((256, blocks * 128), BF16),
            ((144, blocks * 128), BF16),
            ((blocks * 128, 256), BF16),
            ((5 * blocks, 128), F32),
            ((6 * blocks, 128), F32),
        ],
        gas, cell, tile, count, frac, mass, vel, temp, to_near,
        loose=(8,), flops=1 << 32,
    )
    halo, ends = call(
        join_halo, [((384, 128), F32), ends_shape],
        gas, gas_c, gas_d, gas_near, gas_carry, gas_far, gas_turn, part,
        loose=(7,),
    )
    ends = swap_ends(ends)
    sums, ghosts = call(
        deposit, [((960, 128), F32), ends_shape],
        halo, ends, planar, vertical, across, part, drops,
        scratch=[
            pltpu.VMEM((5 * blocks, 128), F32),
            pltpu.VMEM((5 * blocks, 128), F32),
            pltpu.VMEM((960, blocks * 128), BF16),
        ],
    )
    own, sides, to_c, to_d = call(
        fold_z, [((640, 128), F32), ((160, 128), F32), ((80, 128), F32), ((80, 128), F32)],
        sums, swap_ends(ghosts),
    )
    dep_d, dep_c = send(to_d, "D"), send(to_c, "C")
    to_near, to_carry, to_far, to_turn = call(
        fold_y, [((80, 128), F32), ((120, 128), F32), ((80, 128), F32), ((8, 128), F32)],
        sides, dep_c, dep_d,
    )
    dep_near, dep_far = send(to_near, "near"), send(to_far, "far")
    dep_carry = send(to_carry, "carry")
    dep_turn = send(to_turn, "turn")
    base = call(
        stencil, ((640, 128), F32),
        gas, start, halo, ends, own, dep_c, dep_d, to_near,
        loose=(7,), scratch=[pltpu.VMEM((128, 128), F32)], flops=1 << 32,
    )
    out = call(finish, ((640, 128), F32), base, dep_near, dep_carry, dep_far, dep_turn)
    return out.reshape(gas_state.shape)


def solution(mesh):
    in_specs = (
        P(None, "gx", "gy", "gz"),
        P(None, "gx", "gy", "gz"),
        P("gx", "gy", "gz", None, None),
        P("gx", "gy", "gz", None),
        P("gx", "gy", "gz", None),
        P("gx", "gy", "gz", None, None, None),
        P("gx", "gy", "gz", None, None, None),
        P("gx", "gy", "gz", None, None),
        P("gx", "gy", "gz", None, None),
    )
    return jax.shard_map(
        local, mesh=mesh, in_specs=in_specs, out_specs=P(None, "gx", "gy", "gz"), check_vma=False
    )
```

```python
import jax
import jax.numpy as jnp
from jax import lax
from jax.experimental import pallas as pl
from jax.experimental.pallas import tpu as pltpu
from jax.sharding import PartitionSpec as P


PARCEL = 8.0
LATENT = 0.5
TIME_INCREMENT = 0.2
VISCOSITY = 0.5

AXES = ("gx", "gy", "gz")
F32 = jnp.float32
BF16 = jnp.bfloat16
I32 = jnp.int32
FAR_AWAY = -100

OWN = 128
HALO = 64


def swaps(shape):
    nx, ny, nz = shape

    def pairs(target):
        out = []
        for i in range(nx):
            for j in range(ny):
                for k in range(nz):
                    there = target(i, j, k)
                    if there is not None:
                        a, b, c = there
                        out.append(((i * ny + j) * nz + k, (a * ny + b) * nz + c))
        return out

    def d_side(i, j, k):
        if j == 0:
            return (i ^ 1, ny - 1, k)
        if j == ny - 1:
            return (i ^ 1, 0, k)
        return (i, ((j - 1) ^ 1) + 1, k)

    def turn(i, j, k):
        if j in (0, ny - 1):
            return ((i + 2) % nx if i % 2 == 0 else (i - 2) % nx, j, k)
        return None

    return {
        "near": pairs(lambda i, j, k: (i ^ 1, j, k) if 0 < j < ny - 1 else None),
        "carry": pairs(lambda i, j, k: (i ^ 1, j, k) if j in (0, ny - 1) else None),
        "far": pairs(lambda i, j, k: ((i - 1) % nx if i % 2 == 0 else (i + 1) % nx, j, k)),
        "turn": pairs(turn),
        "C": pairs(lambda i, j, k: (i, j ^ 1, k)),
        "D": pairs(d_side),
    }


def places():
    i, j = lax.axis_index("gx"), lax.axis_index("gy")
    odd_i, odd_j = lax.rem(i, 2), lax.rem(j, 2)
    wrap = jnp.logical_or(j == 0, j == lax.axis_size("gy") - 1)
    return odd_i, odd_j, wrap


def rows(start, size, unit):
    return pl.ds(pl.multiple_of(start, unit), size)


def post_ends(ref, low, high):
    k, n = lax.axis_index("gz"), ref.shape[0] // 8
    ref[...] = jnp.zeros(ref.shape, F32)
    ref[rows(lax.rem(k + 1, n) * 8, 8, 8), :] = jnp.concatenate(high, axis=0)
    ref[rows(lax.rem(k + n - 1, n) * 8, 8, 8), :] = jnp.concatenate(low, axis=0)


def get_ends(ref):
    k, n = lax.axis_index("gz"), ref.shape[0] // 8
    below = ref[rows(lax.rem(k + n - 1, n) * 8, 8, 8), :]
    above = ref[rows(lax.rem(k + 1, n) * 8, 8, 8), :]
    return below, above


def choose(cond, yes, no):
    pl.when(cond)(yes)
    pl.when(jnp.logical_not(cond))(no)


def own_ends(gas, low_high):
    low_high[...] = jnp.zeros((16, 128), F32)
    for c in range(5):
        turned = gas[c * OWN : c * OWN + OWN, :].T
        low_high[c : c + 1, :] = turned[0:1, :]
        low_high[8 + c : 9 + c, :] = turned[127:128, :]


def pack_x(gas, from_c, from_d, after, to_near, to_carry, to_far, to_turn):
    del after
    odd_i, _, _ = places()
    near = (1 - odd_i) * 7
    to_turn[...] = jnp.zeros((8, 128), F32)
    to_far[80:96, :] = jnp.zeros((16, 128), F32)
    for c in range(5):
        to_far[c * 16 : c * 16 + 16, :] = gas[rows(c * OWN + 112 - near * 16, 16, 16), :]
        to_far[80 + c : 81 + c, :] = from_c[pl.ds(c * 8 + 7 - near, 1), :]
        to_far[88 + c : 89 + c, :] = from_d[pl.ds(c * 8 + 7 - near, 1), :]
        to_turn[c : c + 1, :] = from_d[pl.ds(c * 8 + near, 1), :]
    to_near[80:96, :] = jnp.zeros((16, 128), F32)
    to_carry[120:128, :] = jnp.zeros((8, 128), F32)
    for c in range(5):
        face = gas[rows(c * OWN + near * 16, 16, 16), :]
        to_near[c * 16 : c * 16 + 16, :] = face
        to_near[80 + c : 81 + c, :] = from_c[pl.ds(c * 8 + near, 1), :]
        to_near[88 + c : 89 + c, :] = from_d[pl.ds(c * 8 + near, 1), :]
        to_carry[c * 24 : c * 24 + 16, :] = face
        to_carry[c * 24 + 16 : c * 24 + 24, :] = from_d[c * 8 : c * 8 + 8, :]
        to_carry[120 + c : 121 + c, :] = from_c[pl.ds(c * 8 + near, 1), :]


def join_halo(own, from_c, from_d, from_near, from_carry, from_far, from_turn, after, halo, ends):
    del after
    odd_i, _, wrap = places()
    near = odd_i * 7
    for c in range(5):
        at = c * HALO
        halo[at + 16 : at + 32, :] = from_far[c * 16 : c * 16 + 16, :]
        halo[at + 32 : at + 40, :] = from_c[c * 8 : c * 8 + 8, :]
        halo[at + 40 : at + 48, :] = jnp.zeros((8, 128), F32)
        halo[at + 41 : at + 42, :] = from_far[80 + c : 81 + c, :]
        halo[at + 56 : at + 64, :] = jnp.zeros((8, 128), F32)
    halo[5 * HALO : 384, :] = jnp.zeros((384 - 5 * HALO, 128), F32)

    def wrapped():
        for c in range(5):
            at = c * HALO
            halo[at : at + 16, :] = from_carry[c * 24 : c * 24 + 16, :]
            halo[at + 40 : at + 41, :] = from_carry[120 + c : 121 + c, :]
            halo[at + 48 : at + 56, :] = from_carry[c * 24 + 16 : c * 24 + 24, :]
            halo[at + 56 : at + 57, :] = from_d[pl.ds(c * 8 + near, 1), :]
            halo[at + 57 : at + 58, :] = from_turn[c : c + 1, :]

    def inner():
        for c in range(5):
            at = c * HALO
            halo[at : at + 16, :] = from_near[c * 16 : c * 16 + 16, :]
            halo[at + 40 : at + 41, :] = from_near[80 + c : 81 + c, :]
            halo[at + 48 : at + 56, :] = from_d[c * 8 : c * 8 + 8, :]
            halo[at + 56 : at + 57, :] = from_near[88 + c : 89 + c, :]
            halo[at + 57 : at + 58, :] = from_far[88 + c : 89 + c, :]

    choose(wrap, wrapped, inner)
    turned = [halo[n * 128 : n * 128 + 128, :].T for n in range(3)]
    post_ends(
        ends,
        [own[0:5, :]] + [t[0:1, :] for t in turned],
        [own[8:13, :]] + [t[127:128, :] for t in turned],
    )


def three(place, anchor, offset):
    low = 0.5 * (0.5 - offset) * (0.5 - offset)
    middle = 0.75 - offset * offset
    high = 0.5 * (0.5 + offset) * (0.5 + offset)
    step = place - anchor
    return jnp.where(step == -1, low, jnp.where(step == 0, middle, jnp.where(step == 1, high, 0.0)))


def weigh(
    gas, cell, tile, count, frac, mass, vel, temp, after, planar, vertical, across, part, drops
):
    del after
    odd_i, odd_j, _ = places()
    blocks = cell.shape[0]
    drops[0:blocks, :] = jnp.exp(jnp.log(mass[...]) * (1.0 / 3.0))
    slot = lax.broadcasted_iota(I32, (1, 128), 1)
    drops[2 * blocks : 5 * blocks, :] = vel[...]
    drops[5 * blocks : 6 * blocks, :] = temp[...]
    near_x, far_x = 8 - 9 * odd_i, 9 * odd_i - 1
    c_y, d_y = 16 - 17 * odd_j, 17 * odd_j - 1
    r = lax.broadcasted_iota(I32, (192, 128), 0)
    q = r & 15
    group = (r >> 4) - 8
    on_y = jnp.where(q < 8, q, jnp.where(q == 8, near_x, jnp.where(q == 9, far_x, FAR_AWAY)))
    place_x = jnp.where(group < 0, r >> 4, jnp.where(group == 0, near_x, jnp.where(group == 1, far_x, on_y)))
    place_y = jnp.where(group == 2, c_y, jnp.where(group == 3, d_y, q))
    s = lax.broadcasted_iota(I32, (256, 128), 0)
    place_z = jnp.where(s < 128, s, jnp.where(s == 128, -1, jnp.where(s == 129, 128, FAR_AWAY)))
    cells = gas[...].astype(BF16)
    for b in range(blocks):
        lanes = slice(b * 128, b * 128 + 128)
        at = cell[b : b + 1, :]
        wx = three(place_x, at >> 10, frac[b : b + 1, :])
        drops[blocks + b : blocks + b + 1, :] = jnp.where(slot < count[0:1, b : b + 1], PARCEL, 0.0).astype(F32)
        wy = three(place_y, ((at >> 7) & 7) + 8 * tile[0:1, b : b + 1], frac[blocks + b : blocks + b + 1, :])
        wz = three(place_z, at & 127, frac[2 * blocks + b : 2 * blocks + b + 1, :])
        flat = (wx * wy).astype(BF16)
        planar[0:192, lanes] = flat
        planar[192:256, lanes] = jnp.zeros((64, 128), BF16)
        vertical[:, lanes] = wz[0:144, :].astype(BF16)
        across[lanes, :] = jnp.concatenate([wz[0:128, :].T, wz[128:256, :].T], axis=1).astype(BF16)
        seen = jnp.dot(cells, wz[0:128, :].astype(BF16), preferred_element_type=F32)
        own = flat[0:128, :].astype(F32)
        for c in range(5):
            part[c * blocks + b : c * blocks + b + 1, :] = jnp.sum(
                seen[c * OWN : c * OWN + OWN, :] * own, axis=0, keepdims=True
            )


def deposit(halo, z_ends, planar, vertical, across, part, drops, sums, ghosts, gas_at, source, weighted):
    blocks = drops.shape[0] // 6
    below, above = get_ends(z_ends)

    def z_rows(v):
        turned = pltpu.roll(v, 64, 1)
        side = jnp.concatenate(
            [v[5:6], turned[5:6], v[6:7], turned[6:7], v[7:8], jnp.zeros((3, 128), F32)], axis=0
        )
        return jnp.concatenate([v, side], axis=1)

    ends = jnp.concatenate([z_rows(below), z_rows(above)], axis=0).astype(BF16)
    at_ends = jnp.dot(ends, planar[...], preferred_element_type=F32)
    around = halo[0 : 5 * HALO, :].astype(BF16)
    for b in range(0, blocks, 2):
        lanes = slice(b * 128, b * 128 + 256)
        seen = jnp.dot(around, vertical[0:128, lanes], preferred_element_type=F32)
        side = planar[128:192, lanes].astype(F32)
        edge = vertical[128:144, lanes].astype(F32)
        ended = at_ends[0:8, lanes] * edge[0:1, :] + at_ends[8:16, lanes] * edge[1:2, :]
        for c in range(5):
            n = c * blocks + b
            row = ended[c : c + 1, :] + jnp.sum(seen[c * HALO : c * HALO + HALO, :] * side, axis=0, keepdims=True)
            gas_at[n : n + 1, :] = part[n : n + 1, :] + row[:, 0:128]
            gas_at[n + 1 : n + 2, :] = part[n + 1 : n + 2, :] + row[:, 128:256]
    d = drops[0:blocks, :]
    live = drops[blocks : 2 * blocks, :]
    warm = gas_at[4 * blocks : 5 * blocks, :] - drops[5 * blocks : 6 * blocks, :]
    soft = jnp.maximum(warm, 0.0) + jnp.log1p(jnp.exp(-jnp.abs(warm)))
    rate = d * jnp.log1p(soft)
    pull = d * gas_at[0:blocks, :]
    source[0:blocks, :] = rate * live
    for m in range(1, 4):
        v = drops[(m + 1) * blocks : (m + 2) * blocks, :]
        u = gas_at[m * blocks : (m + 1) * blocks, :]
        source[m * blocks : (m + 1) * blocks, :] = (rate * v - pull * (u - v)) * live
    source[4 * blocks : 5 * blocks, :] = (-(d * warm) - LATENT * rate) * live
    for b in range(blocks):
        lanes = slice(b * 128, b * 128 + 128)
        flat = planar[0:192, lanes].astype(F32)
        for c in range(5):
            scaled = (flat * source[c * blocks + b : c * blocks + b + 1, :]).astype(BF16)
            weighted[c * OWN : c * OWN + OWN, lanes] = scaled[0:128, :]
            weighted[640 + c * HALO : 640 + c * HALO + HALO, lanes] = scaled[128:192, :]
    low, high = [], []
    for n in range(8):
        size = 128 if n < 7 else 64
        total = jnp.dot(weighted[n * 128 : n * 128 + size, :], across[...], preferred_element_type=F32)
        sums[n * 128 : n * 128 + size, :] = total[:, 0:128]
        ends = total[:, 128:256]
        if size < 128:
            ends = jnp.concatenate([ends, jnp.zeros((128 - size, 128), F32)], axis=0)
        turned = ends.T
        low.append(turned[0:1, :])
        high.append(turned[1:2, :])
    post_ends(ghosts, low, high)


def upright(below, above):
    z = lax.broadcasted_iota(I32, (128, 128), 0)
    return jnp.where(z == 0, below, jnp.where(z == 127, above, 0.0)).T


def fold_z(sums, z_ends, own, sides, to_c, to_d):
    below, above = get_ends(z_ends)
    for n in range(8):
        extra = upright(below[n : n + 1, :], above[n : n + 1, :])
        if n < 5:
            own[n * OWN : n * OWN + OWN, :] = sums[n * OWN : n * OWN + OWN, :] + extra
            continue
        for half in range(2):
            c = (n - 5) * 2 + half
            if c > 4:
                continue
            at = 640 + c * HALO
            here = sums[at : at + HALO, :] + extra[half * 64 : half * 64 + 64, :]
            sides[c * 32 : c * 32 + 32, :] = here[0:32, :]
            to_c[c * 16 : c * 16 + 16, :] = here[32:48, :]
            to_d[c * 16 : c * 16 + 16, :] = here[48:64, :]


def fold_y(sides, from_c, from_d, to_near, to_carry, to_far, to_turn):
    _, odd_j, wrap = places()
    keep = jnp.where(wrap, 0.0, 1.0).astype(F32)
    y = lax.broadcasted_iota(I32, (16, 128), 0)
    c_y = 15 - 15 * odd_j
    at_c, at_d = y == c_y, y == 15 - c_y
    to_turn[...] = jnp.zeros((8, 128), F32)
    for c in range(5):
        for side in range(2):
            row = c * 16 + 8 + side
            folded = (
                sides[c * 32 + side * 16 : c * 32 + side * 16 + 16, :]
                + jnp.where(at_c, from_c[row : row + 1, :], 0.0)
                + jnp.where(at_d, from_d[row : row + 1, :] * keep, 0.0)
            )
            if side == 0:
                to_near[c * 16 : c * 16 + 16, :] = folded
                to_carry[c * 24 : c * 24 + 16, :] = folded
            else:
                to_far[c * 16 : c * 16 + 16, :] = folded
        to_carry[c * 24 + 16 : c * 24 + 24, :] = from_d[c * 16 : c * 16 + 8, :]
        to_turn[c : c + 1, :] = from_d[c * 16 + 9 : c * 16 + 10, :]


def stencil(gas, start, halo, z_ends, own, from_c, from_d, after, out, upper):
    del after
    below, above = get_ends(z_ends)
    odd_i, odd_j, wrap = places()
    keep = jnp.where(wrap, 0.0, 1.0).astype(F32)
    y = lax.broadcasted_iota(I32, (16, 128), 0)
    z = lax.broadcasted_iota(I32, (16, 128), 1)
    c_y = 15 - 15 * odd_j
    at_c, at_d = y == c_y, y == 15 - c_y
    near = (1 - odd_i) * 7
    high_x, low_x = 16 * odd_i, 16 - 16 * odd_i
    high_y, low_y = 32 + 16 * odd_j, 48 - 16 * odd_j
    for c in range(5):
        upper[...] = upright(below[c : c + 1, :], above[c : c + 1, :])
        for x in range(8):
            at = c * OWN + x * 16
            g = gas[at : at + 16, :]
            if x < 7:
                x_up = gas[at + 16 : at + 32, :]
            else:
                x_up = halo[rows(c * HALO + high_x, 16, 16), :]
            if x > 0:
                x_down = gas[at - 16 : at, :]
            else:
                x_down = halo[rows(c * HALO + low_x, 16, 16), :]
            y_up = jnp.where(y == 15, halo[pl.ds(c * HALO + high_y + x, 1), :], pltpu.roll(g, 15, 0))
            y_down = jnp.where(y == 0, halo[pl.ds(c * HALO + low_y + x, 1), :], pltpu.roll(g, 1, 0))
            ends = upper[x * 16 : x * 16 + 16, :]
            z_up = jnp.where(z == 127, ends, pltpu.roll(g, 127, 1))
            z_down = jnp.where(z == 0, ends, pltpu.roll(g, 1, 1))
            laplace = -6.0 * g + (x_up + x_down) + (y_up + y_down) + (z_up + z_down)
            advect = 0.5 * (
                gas[OWN + x * 16 : OWN + x * 16 + 16, :] * (x_up - x_down)
                + gas[2 * OWN + x * 16 : 2 * OWN + x * 16 + 16, :] * (y_up - y_down)
                + gas[3 * OWN + x * 16 : 3 * OWN + x * 16 + 16, :] * (z_up - z_down)
            )
            across = jnp.where(wrap & (near == x), 1.0, 0.0).astype(F32)
            added = (
                own[at : at + 16, :]
                + jnp.where(at_c, from_c[c * 16 + x : c * 16 + x + 1, :], 0.0)
                + jnp.where(
                    at_d,
                    from_d[c * 16 + x : c * 16 + x + 1, :] * keep + from_d[c * 16 + 8 : c * 16 + 9, :] * across,
                    0.0,
                )
            )
            out[at : at + 16, :] = 0.75 * start[at : at + 16, :] + 0.25 * (
                g + TIME_INCREMENT * (VISCOSITY * laplace - advect + added)
            )


def finish(base, from_near, from_carry, from_far, from_turn, out):
    odd_i, odd_j, wrap = places()
    near = (1 - odd_i) * 112
    scale = 0.25 * TIME_INCREMENT
    gate = jnp.where(wrap, scale, 0.0).astype(F32)
    at_d = lax.broadcasted_iota(I32, (16, 128), 0) == 15 * odd_j
    out[...] = base[...]
    for c in range(5):
        at = rows(c * OWN + near, 16, 16)
        out[at, :] = out[at, :] + scale * (
            from_near[c * 16 : c * 16 + 16, :] + from_carry[c * 24 : c * 24 + 16, :]
        )
        at = rows(c * OWN + 112 - near, 16, 16)
        turned = jnp.where(at_d, from_turn[c : c + 1, :] * gate, 0.0)
        out[at, :] = out[at, :] + scale * from_far[c * 16 : c * 16 + 16, :] + turned

    def across(y):
        def add():
            for c in range(5):
                at = pl.ds(c * OWN + y, 8, stride=16)
                out[at, :] = out[at, :] + scale * from_carry[c * 24 + 16 : c * 24 + 24, :]

        return add

    pl.when(wrap & (odd_j == 0))(across(0))
    pl.when(wrap & (odd_j == 1))(across(15))


def call(body, out_shapes, *operands, loose=(), scratch=(), flops=10000):
    whole = pl.BlockSpec(memory_space=pltpu.VMEM)
    anywhere = pl.BlockSpec(memory_space=pl.ANY)
    single = not isinstance(out_shapes, list)
    outs = [out_shapes] if single else out_shapes
    result = pl.pallas_call(
        body,
        out_shape=[jax.ShapeDtypeStruct(s, t) for s, t in outs],
        in_specs=[anywhere if n in loose else whole for n in range(len(operands))],
        out_specs=[whole] * len(outs),
        scratch_shapes=list(scratch),
        compiler_params=pltpu.CompilerParams(vmem_limit_bytes=24 * 1024 * 1024),
        cost_estimate=pl.CostEstimate(flops=flops, bytes_accessed=100000, transcendentals=0),
    )(*operands)
    return result[0] if single else result


def local(gas_state, section_start, drop_cell, block_tile, droplets_per_block, drop_frac, drop_vel, drop_mass, drop_temp):
    shape = tuple(lax.axis_size(a) for a in AXES)
    routes = swaps(shape)

    def send(values, route):
        return lax.ppermute(values, AXES, routes[route])

    def swap_ends(values):
        chunks = values.reshape(shape[2], 8, 128)
        return lax.all_to_all(chunks, "gz", 0, 0).reshape(values.shape)

    blocks = drop_cell.shape[3]
    ends_shape = ((8 * shape[2], 128), F32)
    gas = gas_state.reshape(640, 128)
    start = section_start.reshape(640, 128)
    cell = drop_cell.reshape(blocks, 128)
    frac = drop_frac.reshape(3 * blocks, 128)
    vel = drop_vel.reshape(3 * blocks, 128)
    temp = drop_temp.reshape(blocks, 128)
    mass = drop_mass.reshape(blocks, 128)
    count = droplets_per_block.reshape(1, blocks)
    tile = block_tile.reshape(1, blocks)

    odd_j = lax.rem(lax.axis_index("gy"), 2)
    low, high = gas_state[:, :, 0, :].reshape(40, 128), gas_state[:, :, 15, :].reshape(40, 128)
    to_c, to_d = jnp.where(odd_j == 0, high, low), jnp.where(odd_j == 0, low, high)
    own_z = call(own_ends, ((16, 128), F32), gas, flops=1 << 32)
    gas_d, gas_c = send(to_d, "D"), send(to_c, "C")
    to_near, to_carry, to_far, to_turn = call(
        pack_x, [((96, 128), F32), ((128, 128), F32), ((96, 128), F32), ((8, 128), F32)],
        gas, gas_c, gas_d, own_z,
        loose=(3,),
    )
    gas_near, gas_far = send(to_near, "near"), send(to_far, "far")
    gas_carry = send(to_carry, "carry")
    gas_turn = send(to_turn, "turn")
    planar, vertical, across, part, drops = call(
        weigh,
        [
            ((256, blocks * 128), BF16),
            ((144, blocks * 128), BF16),
            ((blocks * 128, 256), BF16),
            ((5 * blocks, 128), F32),
            ((6 * blocks, 128), F32),
        ],
        gas, cell, tile, count, frac, mass, vel, temp, to_near,
        loose=(8,), flops=1 << 32,
    )
    halo, ends = call(
        join_halo, [((384, 128), F32), ends_shape],
        own_z, gas_c, gas_d, gas_near, gas_carry, gas_far, gas_turn, part,
        loose=(7,),
    )
    ends = swap_ends(ends)
    sums, ghosts = call(
        deposit, [((960, 128), F32), ends_shape],
        halo, ends, planar, vertical, across, part, drops,
        scratch=[
            pltpu.VMEM((5 * blocks, 128), F32),
            pltpu.VMEM((5 * blocks, 128), F32),
            pltpu.VMEM((960, blocks * 128), BF16),
        ],
    )
    own, sides, to_c, to_d = call(
        fold_z, [((640, 128), F32), ((160, 128), F32), ((80, 128), F32), ((80, 128), F32)],
        sums, swap_ends(ghosts),
    )
    dep_d, dep_c = send(to_d, "D"), send(to_c, "C")
    to_near, to_carry, to_far, to_turn = call(
        fold_y, [((80, 128), F32), ((120, 128), F32), ((80, 128), F32), ((8, 128), F32)],
        sides, dep_c, dep_d,
    )
    dep_near, dep_far = send(to_near, "near"), send(to_far, "far")
    dep_carry = send(to_carry, "carry")
    dep_turn = send(to_turn, "turn")
    base = call(
        stencil, ((640, 128), F32),
        gas, start, halo, ends, own, dep_c, dep_d, to_near,
        loose=(7,), scratch=[pltpu.VMEM((128, 128), F32)], flops=1 << 32,
    )
    out = call(finish, ((640, 128), F32), base, dep_near, dep_carry, dep_far, dep_turn)
    return out.reshape(gas_state.shape)


def solution(mesh):
    in_specs = (
        P(None, "gx", "gy", "gz"),
        P(None, "gx", "gy", "gz"),
        P("gx", "gy", "gz", None, None),
        P("gx", "gy", "gz", None),
        P("gx", "gy", "gz", None),
        P("gx", "gy", "gz", None, None, None),
        P("gx", "gy", "gz", None, None, None),
        P("gx", "gy", "gz", None, None),
        P("gx", "gy", "gz", None, None),
    )
    return jax.shard_map(
        local, mesh=mesh, in_specs=in_specs, out_specs=P(None, "gx", "gy", "gz"), check_vma=False
    )
```
